32 devices in a mesh: rows: 32 (over z, y, x, core).
Axes of the slice: x: 2, y: 2, z: 4, core: 2. Of those that a mesh axis runs over, the one named last changes fastest.
Arguments:
- source: float32 [128, 2048], P('rows'), may hold values from -60 to 60
- observed: float32 [128, 2048], P('rows'), may hold values from -4 to 4
- precision: float32 [128, 2048], P('rows'), may hold values from 1 to 10
- conductivity: float32 [128, 2048], P('rows'), may hold values from 0.5 to 2
- log_field: float32 [16, 128, 2048], P(None, 'rows'), may hold values from -4 to 4
- noise_field: float32 [16, 128, 2048], P(None, 'rows'), may hold values from -6 to 6
- subspace_noise: float32 [16, 256], replicated, may hold values from -6 to 6
- eigenvalues: float32 [256], replicated, may hold values from 0.1 to 100
- basis: bfloat16 [256, 128, 2048], P(None, 'rows'), may hold values from -0.0234375 to 0.0234375
Outputs:
- proposal: float32 [16, 128, 2048], P(None, 'rows')
- new_coef: float32 [16, 256], replicated
The draws below stay inside these ranges and needn't reach their ends.
All inputs are finite; a program needn't handle non-finite values.
Results may differ from the reference program's by a relative error of at most 0.0003.
The reference program's roundings to bfloat16 on the way (of `correction`) count: a program that leaves them out, or rounds other values in their place, can miss the bound.
Values sent between devices are 32-bit elements; how exact they have to be, the bound alone decides.
No kernel may reach another device: no remote copies, remote signals or barrier semaphores. Data moves between devices by JAX's collectives and lax.ppermute only.
A program may use at most 64 MiB of HBM per device.

```python
import math
import jax
import jax.numpy as jnp
from jax import lax

ROWS_DEV = 4
NY = 2048
CHAINS = 16
RANK = 256
ITERS = 4
NX = 128
N_ROWS = 32


def draw_source(key, part):
    positions = jnp.arange(NX, dtype=jnp.float32)[:, None]
    fraction = positions / float(max(NX - 1, 1))
    base = jnp.clip(jax.random.normal(key, (NX, NY), jnp.float32), -6.0, 6.0)
    growth = jnp.exp(jnp.log(5.0) * fraction)
    return base * growth


def raised(entries, own_key, source, target, blocks, factor):
    owner, partner = [(jnp.arange(entries.shape[axis_at]) // (entries.shape[axis_at] // blocks)).reshape([-1 if axis == axis_at else 1 for axis in range(entries.ndim)]) for axis_at in (source, target)]
    chosen = jax.random.permutation(own_key, blocks)[partner]
    strong = (owner == chosen) | (owner == (partner + blocks // 2) % blocks)
    return jnp.where(strong, factor * entries, entries)


def steps_of(own_key, extent, cuts, smallest, high):
    def one(axis_at, parts):
        draws = jax.random.uniform(jax.random.fold_in(jax.random.fold_in(own_key, 6), axis_at), (parts,), jnp.float32, smallest / len(cuts), high / len(cuts))
        return jnp.repeat(jnp.exp(draws), extent[axis_at] // parts).reshape((-1,) + (1,) * (len(extent) - axis_at - 1))

    factor_of = one(*cuts[0])
    for cut in cuts[1:]:
        factor_of = factor_of * one(*cut)
    return factor_of


def noise(key, extent, width, most, cuts=(), held_as=jnp.bfloat16):
    drawn = jax.random.normal(key, extent, jnp.float32) * width
    if len(cuts) > 0:
        drawn = steps_of(key, extent, cuts, -0.22, 0.18) * drawn
    return jnp.clip(drawn, min=-most, max=most).astype(held_as)


def noise_with(own_key, extent, scale, limit, split, heavy, held_as=jnp.bfloat16):
    values = scale * jax.random.normal(own_key, extent, jnp.float32)
    if split:
        values = values * steps_of(own_key, extent, split, -0.22, 0.18)
    return jnp.clip(raised(values, jax.random.fold_in(own_key, 3), *heavy), -limit, limit).astype(held_as)


def setup_inputs(seed: int = 0) -> dict:
    streams_of = jax.random.split(jax.random.key(seed), 10)
    source = draw_source(jax.random.fold_in(streams_of[9], 71), 0)
    observed = noise(streams_of[1], (NX, NY), 0.3, 4.0, ((0, 32),), jnp.float32)
    precision = jnp.clip(jnp.exp(math.log(10.0) - 2.3025851 * jax.random.uniform(streams_of[2], (NX, NY), jnp.float32) ** steps_of(streams_of[2], (NX, NY), ((0, 32),), -0.2, 0.2)), 1.0, 10.0)
    conductivity = jnp.clip(jnp.exp(math.log(2.0) - 1.3862944 * jax.random.uniform(streams_of[3], (NX, NY), jnp.float32) ** steps_of(streams_of[3], (NX, NY), ((0, 32),), -0.2, 0.2)), 0.5, 2.0)
    log_field = noise(streams_of[4], (CHAINS, NX, NY), 0.7, 4.0, ((1, 32),), jnp.float32)
    noise_field = noise(streams_of[5], (CHAINS, NX, NY), 1.0, 6.0, ((1, 32),), jnp.float32)
    subspace_noise = noise(streams_of[6], (CHAINS, RANK), 1.0, 6.0, (), jnp.float32)
    eigenvalues = jnp.clip(jnp.exp(jax.random.uniform(streams_of[7], (RANK,), jnp.float32, math.log(0.1), math.log(100.0))), 0.1, 100.0)
    basis = noise_with(streams_of[8], (RANK, NX, NY), (NX * NY) ** -0.5, 0.0234375, ((1, 32),), (1, 0, 32, 2.75))
    return {"source": source, "observed": observed, "precision": precision, "conductivity": conductivity, "log_field": log_field, "noise_field": noise_field, "subspace_noise": subspace_noise, "eigenvalues": eigenvalues, "basis": basis}


def edge_weights(conductivity):
    padded = jnp.pad(conductivity, 1, mode='edge')
    return (0.5 * (conductivity + padded[:-2, 1:-1]), 0.5 * (conductivity + padded[2:, 1:-1]), 0.5 * (conductivity + padded[1:-1, :-2]), 0.5 * (conductivity + padded[1:-1, 2:]))

def apply_operator(field, weights, diagonal):
    padded = jnp.pad(field, ((0, 0), (1, 1), (1, 1)))
    beside_all = weights[0] * padded[:, :-2, 1:-1] + weights[1] * padded[:, 2:, 1:-1]
    beside_all = beside_all + weights[2] * padded[:, 1:-1, :-2] + weights[3] * padded[:, 1:-1, 2:]
    return diagonal * field - beside_all

def chain_dot(left, right):
    return lax.optimization_barrier(jnp.sum(left * right, axis=(1, 2)))

def broadcast_chain(values):
    return values[:, None, None]

def solve(right_side, weights, diagonal):
    solution = jnp.zeros_like(right_side)
    residual = right_side
    scaled = residual / diagonal
    direction = scaled
    current = chain_dot(residual, scaled)
    for iteration in range(ITERS):
        applied = apply_operator(direction, weights, diagonal)
        step_length = current / chain_dot(direction, applied)
        solution = solution + broadcast_chain(step_length) * direction
        residual = residual - broadcast_chain(step_length) * applied
        scaled = residual / diagonal
        following = chain_dot(residual, scaled)
        direction = scaled + broadcast_chain(following / current) * direction
        current = following
    return solution

def project(fields, basis):
    rounded = fields.astype(jnp.bfloat16)

    def accumulate(block, total):
        start = (block * ROWS_DEV).astype(jnp.int32)
        piece = lax.dynamic_slice_in_dim(rounded, start, ROWS_DEV, 1).astype(jnp.float32)
        basis_rows = lax.dynamic_slice_in_dim(basis, start, ROWS_DEV, 1).astype(jnp.float32)
        return total + jnp.einsum('cxy,rxy->cr', piece, basis_rows, precision=lax.Precision.HIGHEST)
    return lax.fori_loop(jnp.int32(0), jnp.int32(N_ROWS), accumulate, jnp.zeros((fields.shape[0], basis.shape[0]), jnp.float32))

def rebuild(correction, basis):
    weights_f = correction.astype(jnp.float32)

    def one_block(block):
        start = (block * ROWS_DEV).astype(jnp.int32)
        basis_rows = lax.dynamic_slice_in_dim(basis, start, ROWS_DEV, 1).astype(jnp.float32)
        return jnp.einsum('cr,rxy->cxy', weights_f, basis_rows, precision=lax.Precision.HIGHEST)
    blocks = lax.map(one_block, jnp.arange(N_ROWS, dtype=jnp.int32))
    return jnp.transpose(blocks, (1, 0, 2, 3)).reshape(correction.shape[0], NX, NY)

def reference(source, observed, precision, conductivity, log_field, noise_field, subspace_noise, eigenvalues, basis):
    weights = edge_weights(conductivity)
    reaction = jnp.exp(log_field)
    diagonal = weights[0] + weights[1] + weights[2] + weights[3] + reaction
    forward_side = jnp.broadcast_to(source, log_field.shape)
    state = solve(forward_side, weights, diagonal)
    adjoint = solve(precision * (state - observed), weights, diagonal)
    gradient = -reaction * adjoint * state
    chains = log_field.shape[0]
    coefs = project(jnp.concatenate([log_field, noise_field, gradient], 0), basis)
    state_coef = coefs[:chains]
    noise_coef = coefs[chains:2 * chains]
    grad_coef = coefs[2 * chains:]
    variance = 1.0 / (1.0 + eigenvalues)
    keep_factor = (2.0 - 0.8 * variance) / (2.0 + 0.8 * variance)
    drift_factor = 1.6 * variance / (2.0 + 0.8 * variance)
    noise_factor = jnp.sqrt(6.4 * variance) / (2.0 + 0.8 * variance)
    new_coef = keep_factor * state_coef - drift_factor * grad_coef + noise_factor * subspace_noise
    correction = (new_coef - 0.6 * state_coef - 0.8 * noise_coef).astype(jnp.bfloat16)
    proposal = 0.6 * log_field + 0.8 * noise_field + rebuild(correction, basis)
    return (proposal, new_coef)
```

```python
import jax
import jax.numpy as jnp
from jax import lax
from jax.sharding import PartitionSpec as P

ITERS = 4
SHIFTS = (0.0, 0.5, 1.0)
AXIS = "rows"


def shifted(value, step):
    count = lax.axis_size(AXIS)
    pairs = [(i, i + step) for i in range(count) if 0 <= i + step < count]
    return lax.ppermute(value, AXIS, pairs)


def everywhere(value):
    count = lax.axis_size(AXIS)
    return lax.all_to_all(jnp.broadcast_to(value[None], (count,) + value.shape), AXIS, 0, 0)


def neighbours(field, weights):
    up, down, left, right = (weight[1:-1] for weight in weights)
    padded = jnp.pad(field[1:-1], ((0, 0), (0, 0), (1, 1)))
    return up * field[:-2] + down * field[2:] + (left * padded[..., :-2] + right * padded[..., 2:])


def krylov(right_side, inverse, weights):
    halo = ITERS
    rows = right_side.shape[0] - 2 * halo
    vectors, images = [right_side * inverse], []
    for k in range(ITERS):
        inner = tuple(weight[k : weight.shape[0] - k] for weight in weights)
        images.append(neighbours(vectors[-1], inner))
        if k < ITERS - 1:
            vectors.append(images[-1] * inverse[k + 1 : inverse.shape[0] - k - 1])
    vectors = [v[halo - k : halo - k + rows] for k, v in enumerate(vectors)]
    images = [s[halo - k - 1 : halo - k - 1 + rows] for k, s in enumerate(images)]
    return vectors, [right_side[halo : halo + rows]] + images


def differences(sequence, shift):
    out = [sequence[0]]
    while len(sequence) > 1:
        sequence = [b - shift * a for a, b in zip(sequence[:-1], sequence[1:])]
        out.append(sequence[0])
    return out


def moments(vectors, images):
    sums = []
    for shift in SHIFTS:
        u, t = differences(vectors, shift), differences(images, shift)
        for k in range(2 * ITERS):
            sums.append(jnp.sum(u[k // 2] * t[(k + 1) // 2], axis=(0, 2)))
    return jnp.stack(sums)


def coefficients(sums):
    chosen, nearest = None, None
    mean = sums[1] / sums[0]
    for index, shift in enumerate(SHIFTS):
        eta = sums[index * 2 * ITERS : (index + 1) * 2 * ITERS]
        gram = [(1.0 - shift) * eta[k] - eta[k + 1] for k in range(2 * ITERS - 1)]
        low = [[None] * ITERS for _ in range(ITERS)]
        scaled = [[None] * ITERS for _ in range(ITERS)]
        inverse, reduced = [None] * ITERS, [None] * ITERS
        for i in range(ITERS):
            for j in range(i):
                entry = gram[i + j]
                for k in range(j):
                    entry = entry - low[i][k] * scaled[j][k]
                scaled[i][j] = entry
                low[i][j] = entry * inverse[j]
            pivot, target = gram[2 * i], eta[i]
            for k in range(i):
                pivot = pivot - low[i][k] * scaled[i][k]
                target = target - low[i][k] * reduced[k]
            usable = pivot > 1e-6 * gram[2 * i]
            inverse[i] = jnp.where(usable, 1.0 / jnp.where(usable, pivot, 1.0), 0.0)
            reduced[i] = target
        weights = [None] * ITERS
        for i in reversed(range(ITERS)):
            entry = reduced[i] * inverse[i]
            for k in range(i + 1, ITERS):
                entry = entry - low[k][i] * weights[k]
            weights[i] = entry
        for step in range(ITERS - 1):
            for k in range(ITERS - 2, step - 1, -1):
                weights[k] = weights[k] - shift * weights[k + 1]
        distance = jnp.abs(mean - shift)
        if chosen is None:
            chosen, nearest = weights, distance
        else:
            closer = distance < nearest
            chosen = [jnp.where(closer, a, b) for a, b in zip(weights, chosen)]
            nearest = jnp.where(closer, distance, nearest)
    return chosen


def combine(weights, vectors):
    total = weights[0][None, :, None] * vectors[0]
    for weight, vector in zip(weights[1:], vectors[1:]):
        total = total + weight[None, :, None] * vector
    return total


def per_device(
    source,
    observed,
    precision,
    conductivity,
    log_field,
    noise_field,
    subspace_noise,
    eigenvalues,
    basis,
):
    halo = ITERS
    chains, rows, _ = log_field.shape
    rank = basis.shape[0]
    position = lax.axis_index(AXIS)
    devices = lax.axis_size(AXIS)

    shared = jnp.stack([source, conductivity, precision, observed], 1)
    packed = jnp.concatenate([jnp.transpose(log_field, (1, 0, 2)), shared], 1)
    before = shifted(packed[rows - halo :], 1)
    after = shifted(packed[:halo], -1)
    if rows > halo:
        above = shifted(conductivity[rows - halo - 1 : rows - halo], 1)
        below = shifted(conductivity[halo : halo + 1], -1)
    else:
        above = shifted(conductivity[-1:], 2)
        below = shifted(conductivity[:1], -2)
    packed = jnp.concatenate([before, packed, after], 0)
    log_rows = packed[:, :chains]
    source_rows, cond_rows, precision_rows, observed_rows = (
        packed[:, chains + k : chains + k + 1] for k in range(4)
    )
    index = position * rows - halo + jnp.arange(rows + 2 * halo, dtype=jnp.int32)[:, None, None]
    inside = (index >= 0) & (index < devices * rows)
    tall = jnp.concatenate([above[:, None], cond_rows, below[:, None]], 0)
    upper = jnp.where(index == 0, cond_rows, tall[:-2])
    lower = jnp.where(index == devices * rows - 1, cond_rows, tall[2:])
    wide = jnp.pad(cond_rows, ((0, 0), (0, 0), (1, 1)), mode="edge")
    weights = (
        0.5 * (cond_rows + upper),
        0.5 * (cond_rows + lower),
        0.5 * (cond_rows + wide[..., :-2]),
        0.5 * (cond_rows + wide[..., 2:]),
    )
    reaction = jnp.exp(log_rows)
    diagonal = weights[0] + weights[1] + weights[2] + weights[3] + reaction
    inverse = jnp.where(inside, 1.0 / diagonal, 0.0)

    early = jnp.concatenate([log_field, noise_field], 0).astype(jnp.bfloat16)
    early = jnp.einsum("cxy,rxy->cr", early, basis, preferred_element_type=jnp.float32)
    early = early.reshape(devices, -1)

    vectors, images = krylov(source_rows, inverse, weights)
    sums = moments(vectors, images).reshape(-1)
    sent = jnp.concatenate([jnp.broadcast_to(sums, (devices,) + sums.shape), early], 1)
    total = jnp.sum(lax.all_to_all(sent, AXIS, 0, 0), 0)
    sums, early = total[: sums.shape[0]].reshape(-1, chains), total[sums.shape[0] :]
    state = combine(coefficients(sums), vectors)

    state_rows = jnp.concatenate([shifted(state[rows - halo :], 1), state, shifted(state[:halo], -1)], 0)
    side = precision_rows * (state_rows - observed_rows)
    vectors, images = krylov(side, inverse, weights)
    sums = moments(vectors, images).reshape(-1)
    got = everywhere(jnp.concatenate([sums, early]))
    sums, early = jnp.sum(got[:, : sums.shape[0]], 0).reshape(-1, chains), got[:, sums.shape[0] :]
    early = early.reshape(2 * chains, rank)
    adjoint = combine(coefficients(sums), vectors)
    gradient = -reaction[halo : halo + rows] * adjoint * state

    late = jnp.einsum(
        "xcy,rxy->cr", gradient.astype(jnp.bfloat16), basis, preferred_element_type=jnp.float32
    )
    late = jnp.sum(lax.all_to_all(late.reshape(devices, -1), AXIS, 0, 0), 0)
    grad_coef = everywhere(late).reshape(chains, rank)
    state_coef, noise_coef = early[:chains], early[chains:]
    variance = 1.0 / (1.0 + eigenvalues)
    keep_factor = (2.0 - 0.8 * variance) / (2.0 + 0.8 * variance)
    drift_factor = 1.6 * variance / (2.0 + 0.8 * variance)
    noise_factor = jnp.sqrt(6.4 * variance) / (2.0 + 0.8 * variance)
    new_coef = keep_factor * state_coef - drift_factor * grad_coef + noise_factor * subspace_noise
    correction = (new_coef - 0.6 * state_coef - 0.8 * noise_coef).astype(jnp.bfloat16)
    rebuilt = jnp.einsum("cr,rxy->cxy", correction, basis, preferred_element_type=jnp.float32)
    proposal = 0.6 * log_field + 0.8 * noise_field + rebuilt
    return (proposal, new_coef)


def solution(mesh):
    return jax.shard_map(
        per_device,
        mesh=mesh,
        in_specs=(
            P("rows", None),
            P("rows", None),
            P("rows", None),
            P("rows", None),
            P(None, "rows", None),
            P(None, "rows", None),
            P(),
            P(),
            P(None, "rows", None),
        ),
        out_specs=(P(None, "rows", None), P()),
        check_vma=False,
    )
```

```python
import functools

import jax
import jax.numpy as jnp
from jax import lax
from jax.experimental import pallas as pl
from jax.experimental.pallas import tpu as pltpu
from jax.sharding import PartitionSpec as P

ITERS = 4
SHIFTS = (0.0, 0.5, 1.0)
AXIS = "rows"
SUB, LANES = 8, 128
SUMS = 2 * ITERS * len(SHIFTS)


def shifted(value, step):
    count = lax.axis_size(AXIS)
    pairs = [(i, i + step) for i in range(count) if 0 <= i + step < count]
    return lax.ppermute(value, AXIS, pairs)


def exchanged(value):
    return lax.all_to_all(value, AXIS, 0, 0)


def differences(sequence, shift):
    out = [sequence[0]]
    while len(sequence) > 1:
        if shift == 0.0:
            sequence = sequence[1:]
        elif shift == 1.0:
            sequence = [b - a for a, b in zip(sequence[:-1], sequence[1:])]
        else:
            sequence = [b - shift * a for a, b in zip(sequence[:-1], sequence[1:])]
        out.append(sequence[0])
    return out


def coefficients(sums):
    chosen, best = None, None
    for index, shift in enumerate(SHIFTS):
        eta = sums[index * 2 * ITERS : (index + 1) * 2 * ITERS]
        gram = [(1.0 - shift) * eta[k] - eta[k + 1] for k in range(2 * ITERS - 1)]
        low = [[None] * ITERS for _ in range(ITERS)]
        scaled = [[None] * ITERS for _ in range(ITERS)]
        inverse, reduced, quality = [None] * ITERS, [None] * ITERS, None
        for i in range(ITERS):
            for j in range(i):
                entry = gram[i + j]
                for k in range(j):
                    entry = entry - low[i][k] * scaled[j][k]
                scaled[i][j] = entry
                low[i][j] = entry * inverse[j]
            pivot, target = gram[2 * i], eta[i]
            for k in range(i):
                pivot = pivot - low[i][k] * scaled[i][k]
                target = target - low[i][k] * reduced[k]
            size = (1.0 - shift) * eta[2 * i] + jnp.abs(eta[2 * i + 1])
            usable = pivot > 1e-6 * gram[2 * i]
            ratio = jnp.where(usable, pivot, 0.0) / jnp.where(size > 0.0, size, 1.0)
            quality = ratio if quality is None else jnp.minimum(quality, ratio)
            inverse[i] = jnp.where(usable, 1.0 / jnp.where(usable, pivot, 1.0), 0.0)
            reduced[i] = target
        weights = [None] * ITERS
        for i in reversed(range(ITERS)):
            entry = reduced[i] * inverse[i]
            for k in range(i + 1, ITERS):
                entry = entry - low[k][i] * weights[k]
            weights[i] = entry
        if shift != 0.0:
            for step in range(ITERS - 1):
                for k in range(ITERS - 2, step - 1, -1):
                    weights[k] = weights[k] - shift * weights[k + 1]
        if chosen is None:
            chosen, best = weights, quality
        else:
            better = quality > best
            chosen = [jnp.where(better, a, b) for a, b in zip(weights, chosen)]
            best = jnp.where(better, quality, best)
    return chosen


def krylov(rows, groups, vectors, images, inverse, across, along):
    width = across.shape[-1]
    total = rows + 2 * ITERS
    for k in range(ITERS):
        for i in range(total - 2 * (k + 1)):
            at = i + k + 1
            for g in range(groups):
                v = vectors[k][i + 1, g]
                side = across[at]
                beside = pltpu.roll(side * v, 1, 1) + side * pltpu.roll(v, width - 1, 1)
                image = along[at] * vectors[k][i, g] + along[at + 1] * vectors[k][i + 2, g] + beside
                images[k][i, g] = image
                if k < ITERS - 1:
                    vectors[k + 1][i, g] = image * inverse[at, g]


def moment_tile(rows, groups, right_side, vectors, images):
    width = vectors[0].shape[-1]
    lane = lax.broadcasted_iota(jnp.int32, (SUB, LANES), 1)
    tile = jnp.zeros((SUB, LANES), jnp.float32)
    for g in range(groups):

        def one_row(r, totals):
            totals = list(totals)
            for start in range(0, width, LANES):
                cut = pl.ds(start, LANES)
                v = [vectors[k][r + ITERS - k, g, :, cut] for k in range(ITERS)]
                s = [right_side(r, g, cut)]
                s += [images[k][r + ITERS - k - 1, g, :, cut] for k in range(ITERS)]
                for index, shift in enumerate(SHIFTS):
                    u, t = differences(v, shift), differences(s, shift)
                    for m in range(2 * ITERS):
                        slot = index * 2 * ITERS + m
                        totals[slot] = totals[slot] + u[m // 2] * t[(m + 1) // 2]
            return tuple(totals)

        zero = jnp.zeros((SUB, LANES), jnp.float32)
        totals = lax.fori_loop(0, rows, one_row, (zero,) * SUMS)
        for m, total in enumerate(totals):
            tile = jnp.where(lane == g * SUMS + m, jnp.sum(total, 1, keepdims=True), tile)
    return tile


def forward_kernel(
    place,
    log_own,
    log_before,
    log_after,
    own,
    before,
    after,
    far_before,
    far_after,
    early,
    sent,
    kept,
    inverse,
    across,
    along,
    cond,
    side,
    *scratch,
    rows,
    groups,
):
    width = own.shape[-1]
    halo = ITERS
    total = rows + 2 * halo
    vectors, images = scratch[:ITERS], scratch[ITERS:]
    first, last = place[0], place[1]

    def spread(ref, at):
        return jnp.broadcast_to(ref[at : at + 1, :], (SUB, width))

    for i in range(halo):
        cond[1 + i] = jnp.where(first == 0, spread(own, rows), spread(before, rows + rows - halo + i))
        cond[1 + halo + rows + i] = jnp.where(
            last == 0, spread(own, 2 * rows - 1), spread(after, rows + i)
        )
    for i in range(rows):
        cond[1 + halo + i] = spread(own, rows + i)
    cond[0] = jnp.where(first == 1, spread(before, 2 * rows - halo), spread(far_before, 0))
    cond[total + 1] = jnp.where(last == 1, spread(after, rows + halo - 1), spread(far_after, 0))
    column = lax.broadcasted_iota(jnp.int32, (SUB, width), 1)
    for i in range(total + 1):
        along[i] = 0.5 * (cond[i] + cond[i + 1])
    for i in range(total):
        here = cond[i + 1]
        left = jnp.where(column == 0, here, pltpu.roll(here, 1, 1))
        right = jnp.where(column == width - 1, here, pltpu.roll(here, width - 1, 1))
        right = 0.5 * (here + right)
        across[i] = jnp.where(column == width - 1, 0.0, right)
        edges = along[i] + along[i + 1] + 0.5 * (here + left) + right
        if i < halo:
            log, row, shared, outside = log_before, rows - halo + i, before, first == 0
        elif i < halo + rows:
            log, row, shared, outside = log_own, i - halo, own, None
        else:
            log, row, shared, outside = log_after, i - halo - rows, after, last == 0
        source = spread(shared, row)
        if shared is own:
            side[row] = source
        for g in range(groups):
            value = 1.0 / (edges + jnp.exp(log[row, g]))
            if outside is not None:
                value = jnp.where(outside, 0.0, value)
            inverse[i, g] = value
            vectors[0][i, g] = source * value
    krylov(rows, groups, vectors, images, inverse, across, along)
    tile = moment_tile(rows, groups, lambda r, g, cut: side[r, :, cut], vectors, images)
    for d in range(sent.shape[0]):
        sent[d] = early[d] + tile
    for k in range(ITERS):
        for r in range(rows):
            for g in range(groups):
                kept[k, r, g] = vectors[k][r + halo - k, g]


def total_of(got):
    parts = [got[d] for d in range(got.shape[0])]
    while len(parts) > 1:
        parts = [a + b for a, b in zip(parts[::2], parts[1::2])] + parts[len(parts) & ~1 :]
    return parts[0]


def weights_of(tile, g):
    sums = [
        jnp.broadcast_to(tile[:, g * SUMS + m : g * SUMS + m + 1], (SUB, LANES)) for m in range(SUMS)
    ]
    return [weight[:, :1] for weight in coefficients(sums)]


def state_kernel(got, kept, state, early, *, rows, groups):
    tile = total_of(got)
    lane = lax.broadcasted_iota(jnp.int32, (SUB, LANES), 1)
    early[...] = jnp.where(lane < groups * SUMS, 0.0, tile)
    for g in range(groups):
        weights = weights_of(tile, g)
        for r in range(rows):
            value = weights[0] * kept[0, r, g]
            for k in range(1, ITERS):
                value = value + weights[k] * kept[k, r, g]
            state[r, g] = value


def adjoint_kernel(
    state,
    state_before,
    state_after,
    own,
    before,
    after,
    inverse,
    across,
    along,
    early,
    sent,
    kept,
    side,
    *scratch,
    rows,
    groups,
):
    width = own.shape[-1]
    halo = ITERS
    total = rows + 2 * halo
    vectors, images = scratch[:ITERS], scratch[ITERS:]

    def spread(ref, at):
        return jnp.broadcast_to(ref[at : at + 1, :], (SUB, width))

    for i in range(total):
        if i < halo:
            value, row, shared = state_before, i, before
            at = rows - halo + i
        elif i < halo + rows:
            value, row, shared = state, i - halo, own
            at = row
        else:
            value, row, shared = state_after, i - halo - rows, after
            at = row
        precision, observed = spread(shared, 2 * rows + at), spread(shared, 3 * rows + at)
        for g in range(groups):
            right = precision * (value[row, g] - observed)
            if shared is own:
                side[row, g] = right
            vectors[0][i, g] = right * inverse[i, g]
    krylov(rows, groups, vectors, images, inverse, across, along)
    tile = moment_tile(rows, groups, lambda r, g, cut: side[r, g, :, cut], vectors, images)
    sent[...] = jnp.broadcast_to((tile + early[...])[None], sent.shape)
    for k in range(ITERS):
        for r in range(rows):
            for g in range(groups):
                kept[k, r, g] = vectors[k][r + halo - k, g]


def gradient_kernel(got, kept, state, log, gradient, *, rows, groups):
    tile = total_of(got)
    for g in range(groups):
        weights = weights_of(tile, g)
        for r in range(rows):
            value = weights[0] * kept[0, r, g]
            for k in range(1, ITERS):
                value = value + weights[k] * kept[k, r, g]
            value = -jnp.exp(log[r, g]) * value * state[r, g]
            gradient[r, g] = value


def call(kernel, outs, args, scratch=(), scalars=0, **static):
    space = [pl.BlockSpec(memory_space=pltpu.SMEM)] * scalars
    space += [pl.BlockSpec(memory_space=pltpu.VMEM)] * (len(args) - scalars)
    return pl.pallas_call(
        functools.partial(kernel, **static),
        out_shape=[jax.ShapeDtypeStruct(shape, jnp.float32) for shape in outs],
        in_specs=space,
        out_specs=[pl.BlockSpec(memory_space=pltpu.VMEM)] * len(outs),
        scratch_shapes=[pltpu.VMEM(shape, jnp.float32) for shape in scratch],
        compiler_params=pltpu.CompilerParams(vmem_limit_bytes=40 * 1024 * 1024),
    )(*args)


def per_device(
    source,
    observed,
    precision,
    conductivity,
    log_field,
    noise_field,
    subspace_noise,
    eigenvalues,
    basis,
):
    halo = ITERS
    chains, rows, width = log_field.shape
    rank = basis.shape[0]
    groups = chains // SUB
    position = lax.axis_index(AXIS)
    devices = lax.axis_size(AXIS)

    log_rows = jnp.transpose(log_field, (1, 0, 2)).reshape(rows, groups, SUB, width)
    shared = jnp.concatenate([source, conductivity, precision, observed], 0)
    log_before = shifted(log_rows, 1)
    log_after = shifted(log_rows, -1)
    before = shifted(shared, 1)
    after = shifted(shared, -1)
    if rows > halo:
        far_before = before[2 * rows - halo - 1 : 2 * rows - halo]
        far_after = after[rows + halo : rows + halo + 1]
        place = jnp.stack([position, devices - 1 - position]) * 2
    else:
        far_before = shifted(conductivity[rows - 1 :], 2)
        far_after = shifted(conductivity[:1], -2)
        place = jnp.stack([position, devices - 1 - position])

    fields = jnp.transpose(basis, (1, 0, 2))
    early = jnp.concatenate([log_field, noise_field], 0).astype(jnp.bfloat16)
    early = jnp.einsum("cxy,xry->cr", early, fields, preferred_element_type=jnp.float32)
    share = early.size // (devices * SUB)
    early = early.reshape(devices, SUB, share)
    early = jnp.pad(early, ((0, 0), (0, 0), (LANES - share, 0)))

    total = rows + 2 * halo
    block = (groups, SUB, width)
    tiles = (devices, SUB, LANES)
    scratch = [(total - 2 * k,) + block for k in range(ITERS)]
    scratch += [(total - 2 * k - 2,) + block for k in range(ITERS)]
    sent, kept, inverse, across, along = call(
        forward_kernel,
        [
            tiles,
            (ITERS, rows) + block,
            (total,) + block,
            (total, SUB, width),
            (total + 1, SUB, width),
        ],
        [place, log_rows, log_before, log_after, shared, before, after, far_before, far_after, early],
        [(total + 2, SUB, width), (rows, SUB, width)] + scratch,
        scalars=1,
        rows=rows,
        groups=groups,
    )
    state, early = call(
        state_kernel,
        [(rows,) + block, (SUB, LANES)],
        [exchanged(sent), kept],
        rows=rows,
        groups=groups,
    )
    state_before = shifted(state[rows - halo :], 1)
    state_after = shifted(state[:halo], -1)
    sent, kept = call(
        adjoint_kernel,
        [tiles, (ITERS, rows) + block],
        [state, state_before, state_after, shared, before, after, inverse, across, along, early],
        [(rows,) + block] + scratch,
        rows=rows,
        groups=groups,
    )
    got = exchanged(sent)
    (gradient,) = call(
        gradient_kernel,
        [(rows,) + block],
        [got, kept, state, log_rows],
        rows=rows,
        groups=groups,
    )
    early = got[:, :, LANES - share :].reshape(2 * chains, rank)

    late = jnp.einsum(
        "xcy,xry->cr",
        gradient.reshape(rows, chains, width).astype(jnp.bfloat16),
        fields,
        preferred_element_type=jnp.float32,
    )
    late = jnp.sum(exchanged(late.reshape(devices, -1)), 0)
    grad_coef = exchanged(jnp.broadcast_to(late[None], (devices,) + late.shape)).reshape(chains, rank)
    state_coef, noise_coef = early[:chains], early[chains:]
    variance = 1.0 / (1.0 + eigenvalues)
    keep_factor = (2.0 - 0.8 * variance) / (2.0 + 0.8 * variance)
    drift_factor = 1.6 * variance / (2.0 + 0.8 * variance)
    noise_factor = jnp.sqrt(6.4 * variance) / (2.0 + 0.8 * variance)
    new_coef = keep_factor * state_coef - drift_factor * grad_coef + noise_factor * subspace_noise
    correction = (new_coef - 0.6 * state_coef - 0.8 * noise_coef).astype(jnp.bfloat16)
    rebuilt = jnp.einsum("cr,xry->cxy", correction, fields, preferred_element_type=jnp.float32)
    proposal = 0.6 * log_field + 0.8 * noise_field + rebuilt
    return (proposal, new_coef)


def solution(mesh):
    return jax.shard_map(
        per_device,
        mesh=mesh,
        in_specs=(
            P("rows", None),
            P("rows", None),
            P("rows", None),
            P("rows", None),
            P(None, "rows", None),
            P(None, "rows", None),
            P(),
            P(),
            P(None, "rows", None),
        ),
        out_specs=(P(None, "rows", None), P()),
        check_vma=False,
    )
```

```python
import functools
import math

import jax
import jax.numpy as jnp
from jax import lax
from jax.experimental import pallas as pl
from jax.experimental.pallas import tpu as pltpu
from jax.sharding import PartitionSpec as P

ITERS = 4
SHIFTS = (0.0, 0.5, 1.0)
AXIS = "rows"
SUB, LANES = 8, 128
SUMS = 2 * ITERS * len(SHIFTS)


def shifted(value, step):
    count = lax.axis_size(AXIS)
    pairs = [(i, i + step) for i in range(count) if 0 <= i + step < count]
    return lax.ppermute(value, AXIS, pairs)


def exchanged(value):
    return lax.all_to_all(value, AXIS, 0, 0)


def summed(value):
    count = lax.axis_size(AXIS)
    if count & (count - 1):
        return lax.psum(value, AXIS)
    stride = 1
    while stride < count:
        radix = 4 if (count // stride).bit_length() & 1 else 2
        parts = [value]
        for k in range(1, radix):
            parts.append(lax.ppermute(value, AXIS, [(i, i ^ (k * stride)) for i in range(count)]))
        while len(parts) > 1:
            parts = [a + b for a, b in zip(parts[::2], parts[1::2])]
        value = parts[0]
        stride *= radix
    return value


def differences(sequence, shift):
    out = [sequence[0]]
    while len(sequence) > 1:
        if shift == 0.0:
            sequence = sequence[1:]
        elif shift == 1.0:
            sequence = [b - a for a, b in zip(sequence[:-1], sequence[1:])]
        else:
            sequence = [b - shift * a for a, b in zip(sequence[:-1], sequence[1:])]
        out.append(sequence[0])
    return out


def coefficients(sums):
    chosen, best = None, None
    for index, shift in enumerate(SHIFTS):
        eta = sums[index * 2 * ITERS : (index + 1) * 2 * ITERS]
        gram = [(1.0 - shift) * eta[k] - eta[k + 1] for k in range(2 * ITERS - 1)]
        low = [[None] * ITERS for _ in range(ITERS)]
        scaled = [[None] * ITERS for _ in range(ITERS)]
        inverse, reduced, quality = [None] * ITERS, [None] * ITERS, None
        for i in range(ITERS):
            for j in range(i):
                entry = gram[i + j]
                for k in range(j):
                    entry = entry - low[i][k] * scaled[j][k]
                scaled[i][j] = entry
                low[i][j] = entry * inverse[j]
            pivot, target = gram[2 * i], eta[i]
            for k in range(i):
                pivot = pivot - low[i][k] * scaled[i][k]
                target = target - low[i][k] * reduced[k]
            size = (1.0 - shift) * eta[2 * i] + jnp.abs(eta[2 * i + 1])
            usable = pivot > 1e-6 * gram[2 * i]
            ratio = jnp.where(usable, pivot, 0.0) / jnp.where(size > 0.0, size, 1.0)
            quality = ratio if quality is None else jnp.minimum(quality, ratio)
            inverse[i] = jnp.where(usable, 1.0 / jnp.where(usable, pivot, 1.0), 0.0)
            reduced[i] = target
        weights = [None] * ITERS
        for i in reversed(range(ITERS)):
            entry = reduced[i] * inverse[i]
            for k in range(i + 1, ITERS):
                entry = entry - low[k][i] * weights[k]
            weights[i] = entry
        if shift != 0.0:
            for step in range(ITERS - 1):
                for k in range(ITERS - 2, step - 1, -1):
                    weights[k] = weights[k] - shift * weights[k + 1]
        if chosen is None:
            chosen, best = weights, quality
        else:
            better = quality > best
            chosen = [jnp.where(better, a, b) for a, b in zip(weights, chosen)]
            best = jnp.where(better, quality, best)
    return chosen


def krylov(rows, groups, vectors, images, inverse, across, along):
    width = across.shape[-1]
    total = rows + 2 * ITERS
    for k in range(ITERS):
        for i in range(total - 2 * (k + 1)):
            at = i + k + 1
            for g in range(groups):
                v = vectors[k][i + 1, g]
                side = across[at]
                beside = pltpu.roll(side * v, 1, 1) + side * pltpu.roll(v, width - 1, 1)
                image = along[at] * vectors[k][i, g] + along[at + 1] * vectors[k][i + 2, g] + beside
                images[k][i, g] = image
                if k < ITERS - 1:
                    vectors[k + 1][i, g] = image * inverse[at, g]


def moment_tile(rows, groups, right_side, vectors, images):
    width = vectors[0].shape[-1]
    lane = lax.broadcasted_iota(jnp.int32, (SUB, LANES), 1)
    tile = jnp.zeros((SUB, LANES), jnp.float32)
    for g in range(groups):

        def one_row(r, totals):
            totals = list(totals)
            for start in range(0, width, LANES):
                cut = pl.ds(start, LANES)
                v = [vectors[k][r + ITERS - k, g, :, cut] for k in range(ITERS)]
                s = [right_side(r, g, cut)]
                s += [images[k][r + ITERS - k - 1, g, :, cut] for k in range(ITERS)]
                for index, shift in enumerate(SHIFTS):
                    u, t = differences(v, shift), differences(s, shift)
                    for m in range(2 * ITERS):
                        slot = index * 2 * ITERS + m
                        totals[slot] = totals[slot] + u[m // 2] * t[(m + 1) // 2]
            return tuple(totals)

        zero = jnp.zeros((SUB, LANES), jnp.float32)
        totals = lax.fori_loop(0, rows, one_row, (zero,) * SUMS)
        for m, total in enumerate(totals):
            tile = jnp.where(lane == g * SUMS + m, jnp.sum(total, 1, keepdims=True), tile)
    return tile


def forward_kernel(
    place,
    log_own,
    log_before,
    log_after,
    own,
    before,
    after,
    far_before,
    far_after,
    sent,
    kept,
    inverse,
    across,
    along,
    cond,
    side,
    *scratch,
    rows,
    groups,
):
    width = own.shape[-1]
    halo = ITERS
    total = rows + 2 * halo
    vectors, images = scratch[:ITERS], scratch[ITERS:]
    first, last = place[0], place[1]

    def spread(ref, at):
        return jnp.broadcast_to(ref[at : at + 1, :], (SUB, width))

    for i in range(halo):
        cond[1 + i] = jnp.where(first == 0, spread(own, rows), spread(before, rows + rows - halo + i))
        cond[1 + halo + rows + i] = jnp.where(
            last == 0, spread(own, 2 * rows - 1), spread(after, rows + i)
        )
    for i in range(rows):
        cond[1 + halo + i] = spread(own, rows + i)
    cond[0] = jnp.where(first == 1, spread(before, 2 * rows - halo), spread(far_before, 0))
    cond[total + 1] = jnp.where(last == 1, spread(after, rows + halo - 1), spread(far_after, 0))
    column = lax.broadcasted_iota(jnp.int32, (SUB, width), 1)
    for i in range(total + 1):
        along[i] = 0.5 * (cond[i] + cond[i + 1])
    for i in range(total):
        here = cond[i + 1]
        left = jnp.where(column == 0, here, pltpu.roll(here, 1, 1))
        right = jnp.where(column == width - 1, here, pltpu.roll(here, width - 1, 1))
        right = 0.5 * (here + right)
        across[i] = jnp.where(column == width - 1, 0.0, right)
        edges = along[i] + along[i + 1] + 0.5 * (here + left) + right
        if i < halo:
            log, row, shared, outside = log_before, rows - halo + i, before, first == 0
        elif i < halo + rows:
            log, row, shared, outside = log_own, i - halo, own, None
        else:
            log, row, shared, outside = log_after, i - halo - rows, after, last == 0
        source = spread(shared, row)
        if shared is own:
            side[row] = source
        for g in range(groups):
            value = 1.0 / (edges + jnp.exp(log[row, g]))
            if outside is not None:
                value = jnp.where(outside, 0.0, value)
            inverse[i, g] = value
            vectors[0][i, g] = source * value
    krylov(rows, groups, vectors, images, inverse, across, along)
    tile = moment_tile(rows, groups, lambda r, g, cut: side[r, :, cut], vectors, images)
    sent[...] = jnp.broadcast_to(tile[None], sent.shape)
    for k in range(ITERS):
        for r in range(rows):
            for g in range(groups):
                kept[k, r, g] = vectors[k][r + halo - k, g]


def total_of(got):
    parts = [got[d] for d in range(got.shape[0])]
    while len(parts) > 1:
        parts = [a + b for a, b in zip(parts[::2], parts[1::2])] + parts[len(parts) & ~1 :]
    return parts[0]


def weights_of(tile, g):
    sums = [
        jnp.broadcast_to(tile[:, g * SUMS + m : g * SUMS + m + 1], (SUB, LANES)) for m in range(SUMS)
    ]
    return [weight[:, :1] for weight in coefficients(sums)]


def state_kernel(got, kept, own, state, side, token, *, rows, groups):
    tile = total_of(got)
    width = own.shape[-1]
    token[...] = tile
    for g in range(groups):
        weights = weights_of(tile, g)
        for r in range(rows):
            value = weights[0] * kept[0, r, g]
            for k in range(1, ITERS):
                value = value + weights[k] * kept[k, r, g]
            state[r, g] = value
            precision = jnp.broadcast_to(own[2 * rows + r : 2 * rows + r + 1, :], (SUB, width))
            observed = jnp.broadcast_to(own[3 * rows + r : 3 * rows + r + 1, :], (SUB, width))
            side[r, g] = precision * (value - observed)


def adjoint_kernel(
    _, side, side_before, side_after, inverse, across, along, sent, kept, *scratch, rows, groups
):
    halo = ITERS
    total = rows + 2 * halo
    vectors, images = scratch[:ITERS], scratch[ITERS:]
    for i in range(total):
        if i < halo:
            value, row = side_before, i
        elif i < halo + rows:
            value, row = side, i - halo
        else:
            value, row = side_after, i - halo - rows
        for g in range(groups):
            vectors[0][i, g] = value[row, g] * inverse[i, g]
    krylov(rows, groups, vectors, images, inverse, across, along)
    tile = moment_tile(rows, groups, lambda r, g, cut: side[r, g, :, cut], vectors, images)
    sent[...] = jnp.broadcast_to(tile[None], sent.shape)
    for k in range(ITERS):
        for r in range(rows):
            for g in range(groups):
                kept[k, r, g] = vectors[k][r + halo - k, g]


def factors(eigenvalues):
    variance = 1.0 / (1.0 + eigenvalues)
    below = 2.0 + 0.8 * variance
    return (2.0 - 0.8 * variance) / below, 1.6 * variance / below, jnp.sqrt(6.4 * variance) / below


def folded(picked, rows):
    size = picked.shape[1]
    lane = lax.broadcasted_iota(jnp.int32, (size, size // rows), 0)
    to = lax.broadcasted_iota(jnp.int32, (size, size // rows), 1)
    ones = jnp.where((lane >= to * rows) & (lane < to * rows + rows), 1.0, 0.0).astype(jnp.bfloat16)
    total = None
    for _ in range(3):
        part = picked.astype(jnp.bfloat16)
        picked = picked - part.astype(jnp.float32)
        part = jnp.dot(part, ones, preferred_element_type=jnp.float32)
        total = part if total is None else total + part
    return total


def picked_rows(product, rows, chains):
    row = lax.rem(lax.broadcasted_iota(jnp.int32, (chains, product.shape[1]), 1), rows)
    out = product[:chains]
    for x in range(1, rows):
        out = jnp.where(row == x, product[x * chains : (x + 1) * chains], out)
    return out


def across_lanes(left, right):
    return lax.dot_general(left, right, (((1,), (1,)), ((), ())), preferred_element_type=jnp.float32)


def early_kernel(_, basis, log, noise, fields, coefs, buffer, picked, arrived, *, rows, chains, steps):
    ranks = basis.shape[0] // steps
    width = basis.shape[2]
    copies = []
    for j in range(steps):
        part = pl.ds(j * ranks, ranks)
        copies.append(pltpu.make_async_copy(basis.at[part], buffer.at[part], arrived.at[j]))
        copies[-1].start()
    left = jnp.concatenate([log[...].astype(jnp.bfloat16), noise[...]], 0)
    for j in range(steps):
        copies[j].wait()
        block = buffer[pl.ds(j * ranks, ranks)].reshape(ranks * rows, width)
        cut = pl.ds(j * ranks * rows, ranks * rows)
        fields[cut, :] = block
        product = across_lanes(left, block)
        half = rows * chains
        picked[:chains, cut] = picked_rows(product[:half], rows, chains)
        picked[chains:, cut] = picked_rows(product[half:], rows, chains)
    coefs[...] = folded(picked[...], rows)


def gradient_kernel(
    got, kept, state, log, fields, early, eigenvalues, sums, gradient, picked, *, rows, groups
):
    tile = total_of(got)
    chains = groups * SUB
    for g in range(groups):
        weights = weights_of(tile, g)
        for r in range(rows):
            value = weights[0] * kept[0, r, g]
            for k in range(1, ITERS):
                value = value + weights[k] * kept[k, r, g]
            value = -jnp.exp(log[r, g]) * value * state[r, g]
            gradient[r * chains + g * SUB : r * chains + (g + 1) * SUB, :] = value
    left = gradient[...].astype(jnp.bfloat16)
    size = fields.shape[0]
    step = min(size, 2 * LANES)
    for start in range(0, size, step):
        product = across_lanes(left, fields[start : start + step, :])
        picked[:, start : start + step] = picked_rows(product, rows, chains)
    keep, drift, _ = factors(eigenvalues[...])
    state_coef, noise_coef = early[:chains], early[chains:]
    sums[:chains] = keep * state_coef - drift * folded(picked[...], rows)
    sums[chains:] = -0.6 * state_coef - 0.8 * noise_coef


def proposal_kernel(
    sums, eigenvalues, subspace, fields, log, noise, proposal, new_coef, result, sent, *, rows, chains, steps
):
    _, _, noise_factor = factors(eigenvalues[...])
    coef = sums[:chains] + noise_factor * subspace[...]
    new_coef[...] = coef
    correction = (coef + sums[chains:]).astype(jnp.bfloat16)
    size, width = fields.shape
    rank = size // rows
    row = lax.broadcasted_iota(jnp.int32, (chains * rows, chains), 0)
    to = lax.broadcasted_iota(jnp.int32, (chains * rows, chains), 1)
    tall = jnp.where((row >= to * rows) & (row < to * rows + rows), 1.0, 0.0).astype(jnp.bfloat16)
    lane = lax.broadcasted_iota(jnp.int32, (rank, size), 1)
    to = lax.broadcasted_iota(jnp.int32, (rank, size), 0)
    wide = jnp.where((lane >= to * rows) & (lane < to * rows + rows), 1.0, 0.0).astype(jnp.bfloat16)
    left = jnp.dot(tall, correction, preferred_element_type=jnp.float32).astype(jnp.bfloat16)
    left = jnp.dot(left, wide, preferred_element_type=jnp.float32)
    row = lax.rem(lax.broadcasted_iota(jnp.int32, left.shape, 0), rows)
    lane = lax.rem(lax.broadcasted_iota(jnp.int32, left.shape, 1), rows)
    left = jnp.where(row == lane, left, 0.0).astype(jnp.bfloat16)
    copies = []
    for j in range(steps):
        cut = pl.ds(j * (width // steps), width // steps)
        product = jnp.dot(left, fields[:, cut], preferred_element_type=jnp.float32)
        for c in range(chains):
            base = 0.6 * log[c, :, cut] + 0.8 * noise[c, :, cut]
            result[c, :, cut] = base + product[c * rows : (c + 1) * rows]
        copies.append(
            pltpu.make_async_copy(result.at[:, :, cut], proposal.at[:, :, cut], sent.at[j])
        )
        copies[-1].start()
    for copy in copies:
        copy.wait()


def call(kernel, outs, args, scratch=(), spaces=(), out_spaces=(), **static):
    spaces = dict(spaces)
    out_spaces = dict(out_spaces)
    sizes = [math.prod(s) * 4 if isinstance(s, tuple) else 0 for s in scratch]
    limit = sum(sizes) + static.pop("more", 0) + 6 * 1024 * 1024
    outs = [out if len(out) == 2 and not isinstance(out[0], int) else (out, jnp.float32) for out in outs]
    return pl.pallas_call(
        functools.partial(kernel, **static),
        out_shape=[jax.ShapeDtypeStruct(*out) for out in outs],
        in_specs=[pl.BlockSpec(memory_space=spaces.get(i, pltpu.VMEM)) for i in range(len(args))],
        out_specs=[pl.BlockSpec(memory_space=out_spaces.get(i, pltpu.VMEM)) for i in range(len(outs))],
        scratch_shapes=[pltpu.VMEM(s, jnp.float32) if isinstance(s, tuple) else s for s in scratch],
        compiler_params=pltpu.CompilerParams(vmem_limit_bytes=limit),
    )(*args)


def per_device(
    source,
    observed,
    precision,
    conductivity,
    log_field,
    noise_field,
    subspace_noise,
    eigenvalues,
    basis,
):
    halo = ITERS
    chains, rows, width = log_field.shape
    rank = basis.shape[0]
    groups = chains // SUB
    position = lax.axis_index(AXIS)
    devices = lax.axis_size(AXIS)

    targets = jnp.concatenate([source, conductivity, precision, observed], 0)
    shared = targets[: 2 * rows]
    before = shifted(shared, 1)
    after = shifted(shared, -1)
    place = jnp.stack([position, devices - 1 - position])
    if rows > halo:
        far_before = before[2 * rows - halo - 1 : 2 * rows - halo]
        far_after = after[rows + halo : rows + halo + 1]
        place = place * 2
    else:
        far_before = shifted(conductivity[rows - 1 :], 2)
        far_after = shifted(conductivity[:1], -2)
    log_rows = jnp.transpose(log_field, (1, 0, 2)).reshape(rows, groups, SUB, width)
    log_before = shifted(log_rows, 1)
    log_after = shifted(log_rows, -1)

    total = rows + 2 * halo
    block = (groups, SUB, width)
    tiles = (devices, SUB, LANES)
    scratch = [(total - 2 * k,) + block for k in range(ITERS)]
    scratch += [(total - 2 * k - 2,) + block for k in range(ITERS)]
    sent, kept, inverse, across, along = call(
        forward_kernel,
        [
            tiles,
            (ITERS, rows) + block,
            (total,) + block,
            (total, SUB, width),
            (total + 1, SUB, width),
        ],
        [place, log_rows, log_before, log_after, targets, before, after, far_before, far_after],
        [(total + 2, SUB, width), (rows, SUB, width)] + scratch,
        spaces={0: pltpu.SMEM},
        rows=rows,
        groups=groups,
    )
    state, side, token = call(
        state_kernel,
        [(rows,) + block, (rows,) + block, (SUB, LANES)],
        [exchanged(sent), kept, targets],
        rows=rows,
        groups=groups,
    )
    side_before = shifted(side[rows - halo :], 1)
    side_after = shifted(side[:halo], -1)

    noise_rows = jnp.transpose(noise_field, (1, 0, 2)).astype(jnp.bfloat16)
    steps = math.gcd(8, rank)
    fields, early = call(
        early_kernel,
        [((rows * rank, width), jnp.bfloat16), (2 * chains, rank)],
        [
            token,
            basis,
            log_rows.reshape(rows * chains, width),
            noise_rows.reshape(rows * chains, width),
        ],
        [
            pltpu.VMEM(basis.shape, basis.dtype),
            (2 * chains, rows * rank),
            pltpu.SemaphoreType.DMA((steps,)),
        ],
        spaces={1: pltpu.HBM},
        more=basis.size * 2,
        rows=rows,
        chains=chains,
        steps=steps,
    )
    sent, kept = call(
        adjoint_kernel,
        [tiles, (ITERS, rows) + block],
        [early, side, side_before, side_after, inverse, across, along],
        scratch,
        rows=rows,
        groups=groups,
    )
    (sums,) = call(
        gradient_kernel,
        [(2 * chains, rank)],
        [exchanged(sent), kept, state, log_rows, fields, early, eigenvalues[None]],
        [(rows * chains, width), (chains, rows * rank)],
        rows=rows,
        groups=groups,
    )
    steps = math.gcd(4, width // LANES)
    proposal, new_coef = call(
        proposal_kernel,
        [log_field.shape, (chains, rank)],
        [summed(sums), eigenvalues[None], subspace_noise, fields, log_field, noise_field],
        [log_field.shape, pltpu.SemaphoreType.DMA((steps,))],
        out_spaces={0: pl.ANY},
        rows=rows,
        chains=chains,
        steps=steps,
    )
    return (proposal, new_coef)


def solution(mesh):
    return jax.shard_map(
        per_device,
        mesh=mesh,
        in_specs=(
            P("rows", None),
            P("rows", None),
            P("rows", None),
            P("rows", None),
            P(None, "rows", None),
            P(None, "rows", None),
            P(),
            P(),
            P(None, "rows", None),
        ),
        out_specs=(P(None, "rows", None), P()),
        check_vma=False,
    )
```

```python
import functools
import math

import jax
import jax.numpy as jnp
from jax import lax
from jax.experimental import pallas as pl
from jax.experimental.pallas import tpu as pltpu
from jax.sharding import PartitionSpec as P

ITERS = 4
SHIFTS = (0.0, 0.5, 1.0)
AXIS = "rows"
SUB, LANES = 8, 128
SUMS = 2 * ITERS * len(SHIFTS)


def shifted(value, step):
    count = lax.axis_size(AXIS)
    pairs = [(i, i + step) for i in range(count) if 0 <= i + step < count]
    return lax.ppermute(value, AXIS, pairs)


def exchanged(value):
    return lax.all_to_all(value, AXIS, 0, 0)


def summed(value):
    count = lax.axis_size(AXIS)
    if count & (count - 1):
        return lax.psum(value, AXIS)
    stride = 1
    while stride < count:
        radix = 4 if (count // stride).bit_length() & 1 else 2
        parts = [value]
        for k in range(1, radix):
            parts.append(lax.ppermute(value, AXIS, [(i, i ^ (k * stride)) for i in range(count)]))
        while len(parts) > 1:
            parts = [a + b for a, b in zip(parts[::2], parts[1::2])]
        value = parts[0]
        stride *= radix
    return value


def differences(sequence, shift):
    out = [sequence[0]]
    while len(sequence) > 1:
        if shift == 0.0:
            sequence = sequence[1:]
        elif shift == 1.0:
            sequence = [b - a for a, b in zip(sequence[:-1], sequence[1:])]
        else:
            sequence = [b - shift * a for a, b in zip(sequence[:-1], sequence[1:])]
        out.append(sequence[0])
    return out


def coefficients(sums):
    chosen, best = None, None
    for index, shift in enumerate(SHIFTS):
        eta = sums[index * 2 * ITERS : (index + 1) * 2 * ITERS]
        gram = [(1.0 - shift) * eta[k] - eta[k + 1] for k in range(2 * ITERS - 1)]
        low = [[None] * ITERS for _ in range(ITERS)]
        scaled = [[None] * ITERS for _ in range(ITERS)]
        inverse, reduced, quality = [None] * ITERS, [None] * ITERS, None
        for i in range(ITERS):
            for j in range(i):
                entry = gram[i + j]
                for k in range(j):
                    entry = entry - low[i][k] * scaled[j][k]
                scaled[i][j] = entry
                low[i][j] = entry * inverse[j]
            pivot, target = gram[2 * i], eta[i]
            for k in range(i):
                pivot = pivot - low[i][k] * scaled[i][k]
                target = target - low[i][k] * reduced[k]
            size = (1.0 - shift) * eta[2 * i] + jnp.abs(eta[2 * i + 1])
            usable = pivot > 1e-6 * gram[2 * i]
            ratio = jnp.where(usable, pivot, 0.0) / jnp.where(size > 0.0, size, 1.0)
            quality = ratio if quality is None else jnp.minimum(quality, ratio)
            inverse[i] = jnp.where(usable, 1.0 / jnp.where(usable, pivot, 1.0), 0.0)
            reduced[i] = target
        weights = [None] * ITERS
        for i in reversed(range(ITERS)):
            entry = reduced[i] * inverse[i]
            for k in range(i + 1, ITERS):
                entry = entry - low[k][i] * weights[k]
            weights[i] = entry
        if shift != 0.0:
            for step in range(ITERS - 1):
                for k in range(ITERS - 2, step - 1, -1):
                    weights[k] = weights[k] - shift * weights[k + 1]
        if chosen is None:
            chosen, best = weights, quality
        else:
            better = quality > best
            chosen = [jnp.where(better, a, b) for a, b in zip(weights, chosen)]
            best = jnp.where(better, quality, best)
    return chosen


def krylov(vectors, images, inverse, across, along):
    width = across.shape[-1]
    groups = inverse.shape[1]
    for k in range(ITERS - 1):
        for i in range(images[k].shape[0]):
            at = i + k + 1
            for g in range(groups):
                v = vectors[k][i + 1, g]
                side = across[at]
                beside = pltpu.roll(side * v, 1, 1) + side * pltpu.roll(v, width - 1, 1)
                image = along[at] * vectors[k][i, g] + along[at + 1] * vectors[k][i + 2, g] + beside
                images[k][i, g] = image
                vectors[k + 1][i, g] = image * inverse[at, g]


def moment_tile(rows, right_side, vectors, images, thirds, halves, across, along):
    width = across.shape[-1]
    groups = vectors[0].shape[1]
    above = ITERS - 1
    for index, shift in enumerate(SHIFTS):
        for g in range(groups):
            for r in range(rows + 1):
                v = [vectors[k][r + above - k, g] for k in range(ITERS)]
                thirds[index, r, g] = differences(v, shift)[ITERS - 1]
            for r in range(rows):
                u = pltpu.roll(thirds[index, r, g], width - 1, 1)
                u = across[above + r] * u + along[above + r + 1] * thirds[index, r + 1, g]
                halves[index, r, g] = u
    lane = lax.broadcasted_iota(jnp.int32, (SUB, LANES), 1)
    tile = jnp.zeros((SUB, LANES), jnp.float32)
    for g in range(groups):

        def one_row(r, totals):
            totals = list(totals)
            for start in range(0, width, LANES):
                cut = pl.ds(start, LANES)
                v = [vectors[k][r + above - k, g, :, cut] for k in range(ITERS - 1)]
                s = [right_side(r, g, cut)]
                s += [images[k][r + above - k - 1, g, :, cut] for k in range(ITERS - 1)]
                for index, shift in enumerate(SHIFTS):
                    u, t = differences(v, shift), differences(s, shift)
                    u.append(thirds[index, r, g, :, cut])
                    t.append(halves[index, r, g, :, cut])
                    for m in range(2 * ITERS):
                        slot = index * 2 * ITERS + m
                        totals[slot] = totals[slot] + u[m // 2] * t[(m + 1) // 2]
            return tuple(totals)

        zero = jnp.zeros((SUB, LANES), jnp.float32)
        totals = list(lax.fori_loop(0, rows, one_row, (zero,) * SUMS))
        for index, shift in enumerate(SHIFTS):
            last = (index + 1) * 2 * ITERS - 1
            totals[last] = 2.0 * totals[last] - shift * totals[last - 1]
        for m, total in enumerate(totals):
            tile = jnp.where(lane == g * SUMS + m, jnp.sum(total, 1, keepdims=True), tile)
    return (tile + pltpu.roll(pltpu.roll(tile, LANES // 2, 1), SUB // 2, 0))[: SUB // 2]


def forward_kernel(
    place,
    own,
    before,
    after,
    far,
    sent,
    kept,
    inverse,
    across,
    along,
    cond,
    side,
    thirds,
    halves,
    *scratch,
    rows,
    groups,
):
    width = own.shape[-1]
    halo = ITERS
    above = halo - 1
    total = rows + above + halo
    chains = groups * SUB
    vectors, images = scratch[:ITERS], scratch[ITERS:]
    first, last = place[0], place[1]

    def spread(ref, at):
        return jnp.broadcast_to(ref[at : at + 1, :], (SUB, width))

    def at_source(ref, row):
        return spread(ref, ref.shape[0] - 2 * rows + row)

    def at_cond(ref, row):
        return spread(ref, ref.shape[0] - rows + row)

    for i in range(halo):
        cond[i] = jnp.where(first == 0, at_cond(own, 0), at_cond(before, rows - halo + i))
        cond[halo + rows + i] = jnp.where(last == 0, at_cond(own, rows - 1), at_cond(after, i))
    for i in range(rows):
        cond[halo + i] = at_cond(own, i)
    cond[total + 1] = jnp.where(last == 1, at_cond(after, halo - 1), spread(far, 0))
    column = lax.broadcasted_iota(jnp.int32, (SUB, width), 1)
    for i in range(total + 1):
        along[i] = 0.5 * (cond[i] + cond[i + 1])
    for i in range(total):
        here = cond[i + 1]
        left = jnp.where(column == 0, here, pltpu.roll(here, 1, 1))
        right = jnp.where(column == width - 1, here, pltpu.roll(here, width - 1, 1))
        right = 0.5 * (here + right)
        across[i] = jnp.where(column == width - 1, 0.0, right)
        edges = along[i] + along[i + 1] + 0.5 * (here + left) + right
        if i < above:
            ref, at, row, outside = before, i, rows - above + i, first == 0
        elif i < above + rows:
            ref, at, row, outside = own, i - above, i - above, None
        else:
            ref, at, row, outside = after, i - above - rows, i - above - rows, last == 0
        source = at_source(ref, row)
        if ref is own:
            side[row] = source
        for g in range(groups):
            start = at * chains + g * SUB
            value = 1.0 / (edges + jnp.exp(ref[start : start + SUB, :]))
            if outside is not None:
                value = jnp.where(outside, 0.0, value)
            inverse[i, g] = value
            vectors[0][i, g] = source * value
    krylov(vectors, images, inverse, across, along)
    tile = moment_tile(
        rows, lambda r, g, cut: side[r, :, cut], vectors, images, thirds, halves, across, along
    )
    sent[...] = jnp.broadcast_to(tile[None], sent.shape)
    for k in range(ITERS):
        for r in range(rows):
            for g in range(groups):
                kept[k, r, g] = vectors[k][r + above - k, g]


def total_of(got):
    parts = [got[d] for d in range(got.shape[0])]
    while len(parts) > 1:
        parts = [a + b for a, b in zip(parts[::2], parts[1::2])] + parts[len(parts) & ~1 :]
    return jnp.concatenate([parts[0], pltpu.roll(parts[0], LANES // 2, 1)], 0)


def weights_of(tile, g):
    sums = [
        jnp.broadcast_to(tile[:, g * SUMS + m : g * SUMS + m + 1], (SUB, LANES)) for m in range(SUMS)
    ]
    return [weight[:, :1] for weight in coefficients(sums)]


def state_kernel(got, kept, precision, observed, state, side, token, *, rows, groups):
    tile = total_of(got)
    width = precision.shape[-1]
    token[...] = tile
    for g in range(groups):
        weights = weights_of(tile, g)
        for r in range(rows):
            value = weights[0] * kept[0, r, g]
            for k in range(1, ITERS):
                value = value + weights[k] * kept[k, r, g]
            state[r, g] = value
            scale = jnp.broadcast_to(precision[r : r + 1, :], (SUB, width))
            side[r, g] = scale * (value - jnp.broadcast_to(observed[r : r + 1, :], (SUB, width)))


def adjoint_kernel(
    _,
    side,
    side_before,
    side_after,
    inverse,
    across,
    along,
    sent,
    kept,
    thirds,
    halves,
    *scratch,
    rows,
    groups,
):
    above = ITERS - 1
    vectors, images = scratch[:ITERS], scratch[ITERS:]
    for i in range(inverse.shape[0]):
        if i < above:
            value, row = side_before, i
        elif i < above + rows:
            value, row = side, i - above
        else:
            value, row = side_after, i - above - rows
        for g in range(groups):
            vectors[0][i, g] = value[row, g] * inverse[i, g]
    krylov(vectors, images, inverse, across, along)
    tile = moment_tile(
        rows, lambda r, g, cut: side[r, g, :, cut], vectors, images, thirds, halves, across, along
    )
    sent[...] = jnp.broadcast_to(tile[None], sent.shape)
    for k in range(ITERS):
        for r in range(rows):
            for g in range(groups):
                kept[k, r, g] = vectors[k][r + above - k, g]


def factors(eigenvalues):
    variance = 1.0 / (1.0 + eigenvalues)
    below = 2.0 + 0.8 * variance
    return (2.0 - 0.8 * variance) / below, 1.6 * variance / below, jnp.sqrt(6.4 * variance) / below


def folded(picked, rows):
    size = picked.shape[1]
    lane = lax.broadcasted_iota(jnp.int32, (size, size // rows), 0)
    to = lax.broadcasted_iota(jnp.int32, (size, size // rows), 1)
    ones = jnp.where((lane >= to * rows) & (lane < to * rows + rows), 1.0, 0.0).astype(jnp.bfloat16)
    total = None
    for _ in range(3):
        part = picked.astype(jnp.bfloat16)
        picked = picked - part.astype(jnp.float32)
        part = jnp.dot(part, ones, preferred_element_type=jnp.float32)
        total = part if total is None else total + part
    return total


def picked_rows(product, rows, chains):
    row = lax.rem(lax.broadcasted_iota(jnp.int32, (chains, product.shape[1]), 1), rows)
    out = product[:chains]
    for x in range(1, rows):
        out = jnp.where(row == x, product[x * chains : (x + 1) * chains], out)
    return out


def across_lanes(left, right):
    return lax.dot_general(left, right, (((1,), (1,)), ((), ())), preferred_element_type=jnp.float32)


def early_kernel(_, basis, log, noise, fields, coefs, buffer, picked, arrived, *, rows, chains, steps):
    ranks = basis.shape[0] // steps
    width = basis.shape[2]
    copies = []
    for j in range(steps):
        part = pl.ds(j * ranks, ranks)
        copies.append(pltpu.make_async_copy(basis.at[part], buffer.at[part], arrived.at[j]))
        copies[-1].start()
    left = jnp.concatenate([log[: rows * chains, :].astype(jnp.bfloat16), noise[...]], 0)
    for j in range(steps):
        copies[j].wait()
        block = buffer[pl.ds(j * ranks, ranks)].reshape(ranks * rows, width)
        cut = pl.ds(j * ranks * rows, ranks * rows)
        fields[cut, :] = block
        product = across_lanes(left, block)
        half = rows * chains
        picked[:chains, cut] = picked_rows(product[:half], rows, chains)
        picked[chains:, cut] = picked_rows(product[half:], rows, chains)
    coefs[...] = folded(picked[...], rows)


def gradient_kernel(
    got, kept, state, log, fields, early, eigenvalues, sums, gradient, picked, *, rows, groups
):
    tile = total_of(got)
    chains = groups * SUB
    for g in range(groups):
        weights = weights_of(tile, g)
        for r in range(rows):
            value = weights[0] * kept[0, r, g]
            for k in range(1, ITERS):
                value = value + weights[k] * kept[k, r, g]
            at = r * chains + g * SUB
            value = -jnp.exp(log[at : at + SUB, :]) * value * state[r, g]
            gradient[at : at + SUB, :] = value
    left = gradient[...].astype(jnp.bfloat16)
    size = fields.shape[0]
    step = min(size, 2 * LANES)
    for start in range(0, size, step):
        product = across_lanes(left, fields[start : start + step, :])
        picked[:, start : start + step] = picked_rows(product, rows, chains)
    keep, drift, _ = factors(eigenvalues[...])
    state_coef, noise_coef = early[:chains], early[chains:]
    sums[:chains] = keep * state_coef - drift * folded(picked[...], rows)
    sums[chains:] = -0.6 * state_coef - 0.8 * noise_coef


def proposal_kernel(
    sums, eigenvalues, subspace, fields, log, noise, proposal, new_coef, result, sent, *, rows, chains, steps
):
    _, _, noise_factor = factors(eigenvalues[...])
    coef = sums[:chains] + noise_factor * subspace[...]
    new_coef[...] = coef
    correction = (coef + sums[chains:]).astype(jnp.bfloat16)
    size, width = fields.shape
    rank = size // rows
    row = lax.broadcasted_iota(jnp.int32, (chains * rows, chains), 0)
    to = lax.broadcasted_iota(jnp.int32, (chains * rows, chains), 1)
    tall = jnp.where((row >= to * rows) & (row < to * rows + rows), 1.0, 0.0).astype(jnp.bfloat16)
    lane = lax.broadcasted_iota(jnp.int32, (rank, size), 1)
    to = lax.broadcasted_iota(jnp.int32, (rank, size), 0)
    wide = jnp.where((lane >= to * rows) & (lane < to * rows + rows), 1.0, 0.0).astype(jnp.bfloat16)
    left = jnp.dot(tall, correction, preferred_element_type=jnp.float32).astype(jnp.bfloat16)
    left = jnp.dot(left, wide, preferred_element_type=jnp.float32)
    row = lax.rem(lax.broadcasted_iota(jnp.int32, left.shape, 0), rows)
    lane = lax.rem(lax.broadcasted_iota(jnp.int32, left.shape, 1), rows)
    left = jnp.where(row == lane, left, 0.0).astype(jnp.bfloat16)
    copies = []
    for j in range(steps):
        cut = pl.ds(j * (width // steps), width // steps)
        product = jnp.dot(left, fields[:, cut], preferred_element_type=jnp.float32)
        for c in range(chains):
            base = 0.6 * log[c, :, cut] + 0.8 * noise[c, :, cut]
            result[c, :, cut] = base + product[c * rows : (c + 1) * rows]
        copies.append(
            pltpu.make_async_copy(result.at[:, :, cut], proposal.at[:, :, cut], sent.at[j])
        )
        copies[-1].start()
    for copy in copies:
        copy.wait()


def call(kernel, outs, args, scratch=(), spaces=(), out_spaces=(), **static):
    spaces = dict(spaces)
    out_spaces = dict(out_spaces)
    sizes = [math.prod(s) * 4 if isinstance(s, tuple) else 0 for s in scratch]
    limit = sum(sizes) + static.pop("more", 0) + 6 * 1024 * 1024
    outs = [out if len(out) == 2 and not isinstance(out[0], int) else (out, jnp.float32) for out in outs]
    return pl.pallas_call(
        functools.partial(kernel, **static),
        out_shape=[jax.ShapeDtypeStruct(*out) for out in outs],
        in_specs=[pl.BlockSpec(memory_space=spaces.get(i, pltpu.VMEM)) for i in range(len(args))],
        out_specs=[pl.BlockSpec(memory_space=out_spaces.get(i, pltpu.VMEM)) for i in range(len(outs))],
        scratch_shapes=[pltpu.VMEM(s, jnp.float32) if isinstance(s, tuple) else s for s in scratch],
        compiler_params=pltpu.CompilerParams(vmem_limit_bytes=limit),
    )(*args)


def per_device(
    source,
    observed,
    precision,
    conductivity,
    log_field,
    noise_field,
    subspace_noise,
    eigenvalues,
    basis,
):
    halo = ITERS
    chains, rows, width = log_field.shape
    rank = basis.shape[0]
    groups = chains // SUB
    position = lax.axis_index(AXIS)
    devices = lax.axis_size(AXIS)

    above = halo - 1
    if rows > halo:
        far = shifted(conductivity[halo : halo + 1], -1)
        place = jnp.stack([position, devices - 1 - position]) * 2
    else:
        far = shifted(conductivity[:1], -2)
        place = jnp.stack([position, devices - 1 - position])
    log_rows = jnp.transpose(log_field, (1, 0, 2)).reshape(rows * chains, width)
    packed = jnp.concatenate([log_rows, source, conductivity], 0)
    before = shifted(packed[(rows - above) * chains :], 1)
    if rows > halo:
        after = shifted(jnp.concatenate([packed[: halo * chains], packed[rows * chains :]], 0), -1)
    else:
        after = shifted(packed, -1)

    total = rows + above + halo
    block = (groups, SUB, width)
    tiles = (devices, SUB // 2, LANES)
    scratch = [(len(SHIFTS), rows + 1) + block, (len(SHIFTS), rows) + block]
    scratch += [(total - 2 * k,) + block for k in range(ITERS)]
    scratch += [(total - 2 * k - 2,) + block for k in range(ITERS - 1)]
    sent, kept, inverse, across, along = call(
        forward_kernel,
        [
            tiles,
            (ITERS, rows) + block,
            (total,) + block,
            (total, SUB, width),
            (total + 1, SUB, width),
        ],
        [place, packed, before, after, far],
        [(total + 2, SUB, width), (rows, SUB, width)] + scratch,
        spaces={0: pltpu.SMEM},
        rows=rows,
        groups=groups,
    )
    state, side, token = call(
        state_kernel,
        [(rows,) + block, (rows,) + block, (SUB, LANES)],
        [exchanged(sent), kept, precision, observed],
        rows=rows,
        groups=groups,
    )
    side_before = shifted(side[rows - above :], 1)
    side_after = shifted(side[:halo], -1)

    noise_rows = jnp.transpose(noise_field, (1, 0, 2)).astype(jnp.bfloat16)
    steps = math.gcd(8, rank)
    fields, early = call(
        early_kernel,
        [((rows * rank, width), jnp.bfloat16), (2 * chains, rank)],
        [
            token,
            basis,
            packed,
            noise_rows.reshape(rows * chains, width),
        ],
        [
            pltpu.VMEM(basis.shape, basis.dtype),
            (2 * chains, rows * rank),
            pltpu.SemaphoreType.DMA((steps,)),
        ],
        spaces={1: pltpu.HBM},
        more=basis.size * 2,
        rows=rows,
        chains=chains,
        steps=steps,
    )
    sent, kept = call(
        adjoint_kernel,
        [tiles, (ITERS, rows) + block],
        [early, side, side_before, side_after, inverse, across, along],
        scratch,
        rows=rows,
        groups=groups,
    )
    (sums,) = call(
        gradient_kernel,
        [(2 * chains, rank)],
        [exchanged(sent), kept, state, packed, fields, early, eigenvalues[None]],
        [(rows * chains, width), (chains, rows * rank)],
        rows=rows,
        groups=groups,
    )
    steps = math.gcd(4, width // LANES)
    proposal, new_coef = call(
        proposal_kernel,
        [log_field.shape, (chains, rank)],
        [summed(sums), eigenvalues[None], subspace_noise, fields, log_field, noise_field],
        [log_field.shape, pltpu.SemaphoreType.DMA((steps,))],
        out_spaces={0: pl.ANY},
        rows=rows,
        chains=chains,
        steps=steps,
    )
    return (proposal, new_coef)


def solution(mesh):
    return jax.shard_map(
        per_device,
        mesh=mesh,
        in_specs=(
            P("rows", None),
            P("rows", None),
            P("rows", None),
            P("rows", None),
            P(None, "rows", None),
            P(None, "rows", None),
            P(),
            P(),
            P(None, "rows", None),
        ),
        out_specs=(P(None, "rows", None), P()),
        check_vma=False,
    )
```

```python
import functools
import math

import jax
import jax.numpy as jnp
from jax import lax
from jax.experimental import pallas as pl
from jax.experimental.pallas import tpu as pltpu
from jax.sharding import PartitionSpec as P

ITERS = 4
SHIFTS = (0.0, 0.5, 1.0)
AXIS = "rows"
SUB, LANES = 8, 128
SUMS = 2 * ITERS * len(SHIFTS)


def shifted(value, step):
    count = lax.axis_size(AXIS)
    pairs = [(i, i + step) for i in range(count) if 0 <= i + step < count]
    return lax.ppermute(value, AXIS, pairs)


def exchanged(value):
    return lax.all_to_all(value, AXIS, 0, 0)


def summed(value):
    count = lax.axis_size(AXIS)
    if count & (count - 1):
        return lax.psum(value, AXIS)
    stride = 1
    while stride < count:
        radix = 4 if (count // stride).bit_length() & 1 else 2
        parts = [value]
        for k in range(1, radix):
            parts.append(lax.ppermute(value, AXIS, [(i, i ^ (k * stride)) for i in range(count)]))
        while len(parts) > 1:
            parts = [a + b for a, b in zip(parts[::2], parts[1::2])]
        value = parts[0]
        stride *= radix
    return value


def differences(sequence, shift):
    out = [sequence[0]]
    while len(sequence) > 1:
        if shift == 0.0:
            sequence = sequence[1:]
        elif shift == 1.0:
            sequence = [b - a for a, b in zip(sequence[:-1], sequence[1:])]
        else:
            sequence = [b - shift * a for a, b in zip(sequence[:-1], sequence[1:])]
        out.append(sequence[0])
    return out


def coefficients(sums):
    chosen, best = None, None
    for index, shift in enumerate(SHIFTS):
        eta = sums[index * 2 * ITERS : (index + 1) * 2 * ITERS]
        gram = [(1.0 - shift) * eta[k] - eta[k + 1] for k in range(2 * ITERS - 1)]
        low = [[None] * ITERS for _ in range(ITERS)]
        scaled = [[None] * ITERS for _ in range(ITERS)]
        inverse, reduced, quality = [None] * ITERS, [None] * ITERS, None
        for i in range(ITERS):
            for j in range(i):
                entry = gram[i + j]
                for k in range(j):
                    entry = entry - low[i][k] * scaled[j][k]
                scaled[i][j] = entry
                low[i][j] = entry * inverse[j]
            pivot, target = gram[2 * i], eta[i]
            for k in range(i):
                pivot = pivot - low[i][k] * scaled[i][k]
                target = target - low[i][k] * reduced[k]
            size = (1.0 - shift) * eta[2 * i] + jnp.abs(eta[2 * i + 1])
            usable = pivot > 1e-6 * gram[2 * i]
            ratio = jnp.where(usable, pivot, 0.0) / jnp.where(size > 0.0, size, 1.0)
            quality = ratio if quality is None else jnp.minimum(quality, ratio)
            inverse[i] = jnp.where(usable, 1.0 / jnp.where(usable, pivot, 1.0), 0.0)
            reduced[i] = target
        weights = [None] * ITERS
        for i in reversed(range(ITERS)):
            entry = reduced[i] * inverse[i]
            for k in range(i + 1, ITERS):
                entry = entry - low[k][i] * weights[k]
            weights[i] = entry
        if shift != 0.0:
            for step in range(ITERS - 1):
                for k in range(ITERS - 2, step - 1, -1):
                    weights[k] = weights[k] - shift * weights[k + 1]
        if chosen is None:
            chosen, best = weights, quality
        else:
            better = quality > best
            chosen = [jnp.where(better, a, b) for a, b in zip(weights, chosen)]
            best = jnp.where(better, quality, best)
    return chosen


def krylov(vectors, images, inverse, across, along):
    width = across.shape[-1]
    groups = inverse.shape[1]
    for k in range(ITERS - 1):
        for i in range(images[k].shape[0]):
            at = i + k + 1
            for g in range(groups):
                v = vectors[k][i + 1, g]
                side = across[at]
                beside = pltpu.roll(side * v, 1, 1) + side * pltpu.roll(v, width - 1, 1)
                image = along[at] * vectors[k][i, g] + along[at + 1] * vectors[k][i + 2, g] + beside
                images[k][i, g] = image
                vectors[k + 1][i, g] = image * inverse[at, g]


def moment_tile(rows, right_side, vectors, images, thirds, halves, across, along):
    width = across.shape[-1]
    groups = vectors[0].shape[1]
    above = ITERS - 1
    for index, shift in enumerate(SHIFTS):
        for g in range(groups):
            for r in range(rows + 1):
                v = [vectors[k][r + above - k, g] for k in range(ITERS)]
                thirds[index, r, g] = differences(v, shift)[ITERS - 1]
            for r in range(rows):
                u = pltpu.roll(thirds[index, r, g], width - 1, 1)
                u = across[above + r] * u + along[above + r + 1] * thirds[index, r + 1, g]
                halves[index, r, g] = u
    lane = lax.broadcasted_iota(jnp.int32, (SUB, LANES), 1)
    tile = jnp.zeros((SUB, LANES), jnp.float32)
    for g in range(groups):

        def one_row(r, totals):
            totals = list(totals)
            for start in range(0, width, LANES):
                cut = pl.ds(start, LANES)
                v = [vectors[k][r + above - k, g, :, cut] for k in range(ITERS - 1)]
                s = [right_side(r, g, cut)]
                s += [images[k][r + above - k - 1, g, :, cut] for k in range(ITERS - 1)]
                for index, shift in enumerate(SHIFTS):
                    u, t = differences(v, shift), differences(s, shift)
                    u.append(thirds[index, r, g, :, cut])
                    t.append(halves[index, r, g, :, cut])
                    for m in range(2 * ITERS):
                        slot = index * 2 * ITERS + m
                        totals[slot] = totals[slot] + u[m // 2] * t[(m + 1) // 2]
            return tuple(totals)

        zero = jnp.zeros((SUB, LANES), jnp.float32)
        totals = list(lax.fori_loop(0, rows, one_row, (zero,) * SUMS))
        for index, shift in enumerate(SHIFTS):
            last = (index + 1) * 2 * ITERS - 1
            totals[last] = 2.0 * totals[last] - shift * totals[last - 1]
        for m, total in enumerate(totals):
            tile = jnp.where(lane == g * SUMS + m, jnp.sum(total, 1, keepdims=True), tile)
    return (tile + pltpu.roll(pltpu.roll(tile, LANES // 2, 1), SUB // 2, 0))[: SUB // 2]


def spread(ref, at):
    return jnp.broadcast_to(ref[at : at + 1, :], (SUB, ref.shape[-1]))


def lateral(here):
    width = here.shape[-1]
    column = lax.broadcasted_iota(jnp.int32, here.shape, 1)
    left = jnp.where(column == 0, here, pltpu.roll(here, 1, 1))
    right = jnp.where(column == width - 1, here, pltpu.roll(here, width - 1, 1))
    right = 0.5 * (here + right)
    return 0.5 * (here + left), right, jnp.where(column == width - 1, 0.0, right)


class Packed:
    def __init__(self, rows, chains):
        self.rows, self.chains = rows, chains
        self.split = (rows - 2) * chains
        self.upward = self.split
        self.downward = (rows - 1) * chains + 2 * rows

    def log(self, row, g):
        at = row * self.chains + g * SUB
        return at if row < self.rows - 2 else at + 2 * self.rows

    def source(self, row):
        return self.split + row

    def cond(self, row):
        return self.split + self.rows + row


def forward_kernel(
    _,
    place,
    own,
    before,
    after,
    far,
    sent,
    v0,
    v1,
    v2,
    v3,
    inverse,
    across,
    along,
    cond,
    side,
    thirds,
    halves,
    *images,
    rows,
    groups,
):
    halo = ITERS
    above = halo - 1
    total = rows + above + halo
    spot = Packed(rows, groups * SUB)
    vectors = (v0, v1, v2, v3)
    first, last = place[0], place[1]
    for i in range(halo):
        at = spot.cond(rows - halo + i)
        cond[i] = jnp.where(first == 0, spread(own, spot.cond(0)), spread(before, at))
        at = spot.cond(i)
        cond[halo + rows + i] = jnp.where(
            last == 0, spread(own, spot.cond(rows - 1)), spread(after, at)
        )
    for i in range(rows):
        cond[halo + i] = spread(own, spot.cond(i))
    cond[total + 1] = jnp.where(last == 1, spread(after, spot.cond(halo - 1)), spread(far, 0))
    for i in range(total + 1):
        along[i] = 0.5 * (cond[i] + cond[i + 1])
    for i in range(total):
        left, right, across[i] = lateral(cond[i + 1])
        edges = along[i] + along[i + 1] + left + right
        if i < above:
            ref, row, outside = before, rows - above + i, first == 0
        elif i < above + rows:
            ref, row, outside = own, i - above, None
        else:
            ref, row, outside = after, i - above - rows, last == 0
        source = spread(ref, spot.source(row))
        if ref is own:
            side[row] = source
        for g in range(groups):
            start = spot.log(row, g)
            value = 1.0 / (edges + jnp.exp(ref[start : start + SUB, :]))
            if outside is not None:
                value = jnp.where(outside, 0.0, value)
            inverse[i, g] = value
            vectors[0][i, g] = source * value
    krylov(vectors, images, inverse, across, along)
    tile = moment_tile(
        rows, lambda r, g, cut: side[r, :, cut], vectors, images, thirds, halves, across, along
    )
    sent[...] = jnp.broadcast_to(tile[None], sent.shape)


def total_of(got):
    parts = [got[d] for d in range(got.shape[0])]
    while len(parts) > 1:
        parts = [a + b for a, b in zip(parts[::2], parts[1::2])] + parts[len(parts) & ~1 :]
    return jnp.concatenate([parts[0], pltpu.roll(parts[0], LANES // 2, 1)], 0)


def weights_of(tile, g):
    sums = [
        jnp.broadcast_to(tile[:, g * SUMS + m : g * SUMS + m + 1], (SUB, LANES)) for m in range(SUMS)
    ]
    return [weight[:, :1] for weight in coefficients(sums)]


def adjoint_kernel(
    place,
    got,
    f0,
    f1,
    f2,
    f3,
    inverse,
    across,
    along,
    before,
    after,
    far_before,
    far_after,
    precision,
    observed,
    sent,
    kept,
    state,
    side,
    outer,
    outer_inverse,
    outer_across,
    outer_along,
    thirds,
    halves,
    *scratch,
    rows,
    groups,
):
    halo = ITERS
    above = halo - 1
    width = across.shape[-1]
    chains = groups * SUB
    spot = Packed(rows, chains)
    first, last = place[0], place[1]
    near = (f0, f1, f2, f3)
    low, high = -above, rows + halo - 1
    new_rows = [low - k for k in (3, 2, 1)] + [high + k for k in (1, 2, 3)]
    slot = {row: i for i, row in enumerate(new_rows)}

    def cond_at(row):
        if row < -rows:
            at = row + 2 * rows
            value = spread(far_before, rows + at)
            return jnp.where(first == 1, spread(before, spot.cond(0)), value) if at == rows - 1 else value
        if row < 0:
            return spread(before, spot.cond(row + rows))
        if row < 2 * rows:
            return spread(after, spot.cond(row - rows))
        return spread(far_after, spot.cond(row - 2 * rows))

    for edge in range(low - 3, low):
        outer_along[edge - low + 3] = 0.5 * (cond_at(edge - 1) + cond_at(edge))
    for edge in range(high + 2, high + 5):
        outer_along[edge - high + 1] = 0.5 * (cond_at(edge - 1) + cond_at(edge))

    def along_at(row):
        if row < low:
            return outer_along[row - low + 3]
        if row > high + 1:
            return outer_along[row - high + 1]
        return along[row - low]

    def across_at(row):
        return outer_across[slot[row]] if row in slot else across[row - low]

    def inverse_at(row, g):
        return outer_inverse[slot[row], g] if row in slot else inverse[row - low, g]

    for row in new_rows:
        left, right, outer_across[slot[row]] = lateral(cond_at(row))
        edges = along_at(row) + along_at(row + 1) + left + right
        for g in range(groups):
            if row < -rows:
                at = row + 2 * rows
                outside, source = first <= 1, spread(far_before, at)
                start = 2 * rows + (at - rows + 2) * chains + g * SUB
                log = far_before[start : start + SUB, :]
            elif row < 0:
                outside, source = first == 0, spread(before, spot.source(row + rows))
                start = spot.log(row + rows, g)
                log = before[start : start + SUB, :]
            else:
                at = row - 2 * rows
                outside, source = last <= 1, spread(far_after, spot.source(at))
                start = spot.log(at, g)
                log = far_after[start : start + SUB, :]
            value = jnp.where(outside, 0.0, 1.0 / (edges + jnp.exp(log)))
            outer_inverse[slot[row], g] = value
            outer[0, slot[row], g] = source * value

    def vector(k, row, g):
        if row < low + k:
            return outer[k, row - low + 3 - k, g]
        if row > high - k:
            return outer[k, row - high + 2 + k, g]
        return near[k][row - low - k, g]

    for k in range(ITERS - 1):
        for i, row in enumerate([low + k + 1 - j for j in (3, 2, 1)] + [high - k - 1 + j for j in (1, 2, 3)]):
            for g in range(groups):
                v, edge = vector(k, row, g), across_at(row)
                image = pltpu.roll(edge * v, 1, 1) + edge * pltpu.roll(v, width - 1, 1)
                image = along_at(row) * vector(k, row - 1, g) + along_at(row + 1) * vector(k, row + 1, g) + image
                outer[k + 1, i, g] = image * inverse_at(row, g)

    vectors, images = scratch[:ITERS], scratch[ITERS:]
    tile = total_of(got)
    for g in range(groups):
        weights = weights_of(tile, g)
        for i in range(high - low + 1):
            row = low + i
            value = weights[0] * vector(0, row, g)
            for k in range(1, ITERS):
                value = value + weights[k] * vector(k, row, g)
            if row < 0:
                at = row + rows
                at = far_before.shape[0] - 2 * rows + at
                scale, target = spread(far_before, at), spread(far_before, at + rows)
            elif row < rows:
                state[row, g] = value
                scale, target = spread(precision, row), spread(observed, row)
            else:
                at = far_after.shape[0] - 2 * rows + row - rows
                scale, target = spread(far_after, at), spread(far_after, at + rows)
            value = scale * (value - target)
            if 0 <= row < rows:
                side[row, g] = value
            vectors[0][i, g] = value * inverse[i, g]
    krylov(vectors, images, inverse, across, along)
    tile = moment_tile(
        rows, lambda r, g, cut: side[r, g, :, cut], vectors, images, thirds, halves, across, along
    )
    sent[...] = jnp.broadcast_to(tile[None], sent.shape)
    for k in range(ITERS):
        for r in range(rows):
            for g in range(groups):
                kept[k, r, g] = vectors[k][r + above - k, g]


def factors(eigenvalues):
    variance = 1.0 / (1.0 + eigenvalues)
    below = 2.0 + 0.8 * variance
    return (2.0 - 0.8 * variance) / below, 1.6 * variance / below, jnp.sqrt(6.4 * variance) / below


def folded(picked, rows):
    size = picked.shape[1]
    lane = lax.broadcasted_iota(jnp.int32, (size, size // rows), 0)
    to = lax.broadcasted_iota(jnp.int32, (size, size // rows), 1)
    ones = jnp.where((lane >= to * rows) & (lane < to * rows + rows), 1.0, 0.0).astype(jnp.bfloat16)
    total = None
    for _ in range(3):
        part = picked.astype(jnp.bfloat16)
        picked = picked - part.astype(jnp.float32)
        part = jnp.dot(part, ones, preferred_element_type=jnp.float32)
        total = part if total is None else total + part
    return total


def picked_rows(product, rows, chains):
    row = lax.rem(lax.broadcasted_iota(jnp.int32, (chains, product.shape[1]), 1), rows)
    out = product[:chains]
    for x in range(1, rows):
        out = jnp.where(row == x, product[x * chains : (x + 1) * chains], out)
    return out


def across_lanes(left, right):
    return lax.dot_general(left, right, (((1,), (1,)), ((), ())), preferred_element_type=jnp.float32)


def early_kernel(basis, own, noise, fields, coefs, picked, *, rows, chains, steps):
    ranks = basis.shape[0] // steps
    width = basis.shape[2]
    spot = Packed(rows, chains)
    log = jnp.concatenate([own[: spot.split, :], own[spot.split + 2 * rows :, :]], 0)
    left = jnp.concatenate([log.astype(jnp.bfloat16), noise[...]], 0)
    for j in range(steps):
        block = basis[pl.ds(j * ranks, ranks)].reshape(ranks * rows, width)
        cut = pl.ds(j * ranks * rows, ranks * rows)
        fields[cut, :] = block
        product = across_lanes(left, block)
        half = rows * chains
        picked[:chains, cut] = picked_rows(product[:half], rows, chains)
        picked[chains:, cut] = picked_rows(product[half:], rows, chains)
    coefs[...] = folded(picked[...], rows)


def gradient_kernel(
    got, kept, state, log, fields, early, eigenvalues, sums, gradient, picked, *, rows, groups
):
    tile = total_of(got)
    chains = groups * SUB
    spot = Packed(rows, chains)
    for g in range(groups):
        weights = weights_of(tile, g)
        for r in range(rows):
            value = weights[0] * kept[0, r, g]
            for k in range(1, ITERS):
                value = value + weights[k] * kept[k, r, g]
            at = spot.log(r, g)
            value = -jnp.exp(log[at : at + SUB, :]) * value * state[r, g]
            at = r * chains + g * SUB
            gradient[at : at + SUB, :] = value
    left = gradient[...].astype(jnp.bfloat16)
    size = fields.shape[0]
    step = min(size, 2 * LANES)
    for start in range(0, size, step):
        product = across_lanes(left, fields[start : start + step, :])
        picked[:, start : start + step] = picked_rows(product, rows, chains)
    keep, drift, _ = factors(eigenvalues[...])
    state_coef, noise_coef = early[:chains], early[chains:]
    sums[:chains] = keep * state_coef - drift * folded(picked[...], rows)
    sums[chains:] = -0.6 * state_coef - 0.8 * noise_coef


def proposal_kernel(
    sums, eigenvalues, subspace, fields, log, noise, proposal, new_coef, result, sent, *, rows, chains, steps
):
    _, _, noise_factor = factors(eigenvalues[...])
    coef = sums[:chains] + noise_factor * subspace[...]
    new_coef[...] = coef
    correction = (coef + sums[chains:]).astype(jnp.bfloat16)
    size, width = fields.shape
    rank = size // rows
    row = lax.broadcasted_iota(jnp.int32, (chains * rows, chains), 0)
    to = lax.broadcasted_iota(jnp.int32, (chains * rows, chains), 1)
    tall = jnp.where((row >= to * rows) & (row < to * rows + rows), 1.0, 0.0).astype(jnp.bfloat16)
    lane = lax.broadcasted_iota(jnp.int32, (rank, size), 1)
    to = lax.broadcasted_iota(jnp.int32, (rank, size), 0)
    wide = jnp.where((lane >= to * rows) & (lane < to * rows + rows), 1.0, 0.0).astype(jnp.bfloat16)
    left = jnp.dot(tall, correction, preferred_element_type=jnp.float32).astype(jnp.bfloat16)
    left = jnp.dot(left, wide, preferred_element_type=jnp.float32)
    row = lax.rem(lax.broadcasted_iota(jnp.int32, left.shape, 0), rows)
    lane = lax.rem(lax.broadcasted_iota(jnp.int32, left.shape, 1), rows)
    left = jnp.where(row == lane, left, 0.0).astype(jnp.bfloat16)
    copies = []
    for j in range(steps):
        cut = pl.ds(j * (width // steps), width // steps)
        product = jnp.dot(left, fields[:, cut], preferred_element_type=jnp.float32)
        for c in range(chains):
            base = 0.6 * log[c, :, cut] + 0.8 * noise[c, :, cut]
            result[c, :, cut] = base + product[c * rows : (c + 1) * rows]
        copies.append(
            pltpu.make_async_copy(result.at[:, :, cut], proposal.at[:, :, cut], sent.at[j])
        )
        copies[-1].start()
    for copy in copies:
        copy.wait()


def call(kernel, outs, args, scratch=(), spaces=(), out_spaces=(), **static):
    spaces = dict(spaces)
    out_spaces = dict(out_spaces)
    sizes = [math.prod(s) * 4 if isinstance(s, tuple) else 0 for s in scratch]
    limit = sum(sizes) + static.pop("more", 0) + 3 * 1024 * 1024
    outs = [out if len(out) == 2 and not isinstance(out[0], int) else (out, jnp.float32) for out in outs]
    return pl.pallas_call(
        functools.partial(kernel, **static),
        out_shape=[jax.ShapeDtypeStruct(*out) for out in outs],
        in_specs=[pl.BlockSpec(memory_space=spaces.get(i, pltpu.VMEM)) for i in range(len(args))],
        out_specs=[pl.BlockSpec(memory_space=out_spaces.get(i, pltpu.VMEM)) for i in range(len(outs))],
        scratch_shapes=[pltpu.VMEM(s, jnp.float32) if isinstance(s, tuple) else s for s in scratch],
        compiler_params=pltpu.CompilerParams(vmem_limit_bytes=limit),
    )(*args)


def per_device(
    source,
    observed,
    precision,
    conductivity,
    log_field,
    noise_field,
    subspace_noise,
    eigenvalues,
    basis,
):
    halo = ITERS
    chains, rows, width = log_field.shape
    rank = basis.shape[0]
    groups = chains // SUB
    position = lax.axis_index(AXIS)
    devices = lax.axis_size(AXIS)

    assert rows == halo and chains % SUB == 0
    above = halo - 1
    spot = Packed(rows, chains)
    far = shifted(conductivity[:1], -2)
    place = jnp.stack([position, devices - 1 - position])
    log_rows = jnp.transpose(log_field, (1, 0, 2)).reshape(rows * chains, width)
    packed = jnp.concatenate(
        [log_rows[: spot.split], source, conductivity, log_rows[spot.split :]], 0
    )
    before = shifted(packed, 1)
    after = shifted(packed, -1)
    noise_rows = jnp.transpose(noise_field, (1, 0, 2)).astype(jnp.bfloat16)
    steps = math.gcd(8, rank)
    fields, early = call(
        early_kernel,
        [((rows * rank, width), jnp.bfloat16), (2 * chains, rank)],
        [
            basis,
            packed,
            noise_rows.reshape(rows * chains, width),
        ],
        [(2 * chains, rows * rank)],
        rows=rows,
        chains=chains,
        steps=steps,
    )
    early, precision, observed = lax.optimization_barrier((early, precision, observed))
    far_before = jnp.concatenate([before[spot.upward :], precision, observed], 0)
    far_after = jnp.concatenate([after[: spot.downward], precision, observed], 0)
    far_before = shifted(far_before, 1)
    far_after = shifted(far_after, -1)

    total = rows + above + halo
    block = (groups, SUB, width)
    tiles = (devices, SUB // 2, LANES)
    moments = [(len(SHIFTS), rows + 1) + block, (len(SHIFTS), rows) + block]
    frames = [(total - 2 * k,) + block for k in range(ITERS)]
    images = [(total - 2 * k - 2,) + block for k in range(ITERS - 1)]
    sent, *vectors, inverse, across, along = call(
        forward_kernel,
        [tiles] + frames + [(total,) + block, (total, SUB, width), (total + 1, SUB, width)],
        [early, place, packed, before, after, far],
        [(total + 2, SUB, width), (rows, SUB, width)] + moments + images,
        spaces={1: pltpu.SMEM},
        rows=rows,
        groups=groups,
    )
    sent, kept, state = call(
        adjoint_kernel,
        [tiles, (ITERS, rows) + block, (rows,) + block],
        [place, exchanged(sent), *vectors, inverse, across, along]
        + [before, after, far_before, far_after, precision, observed],
        [
            (rows,) + block,
            (ITERS, 6) + block,
            (6,) + block,
            (6, SUB, width),
            (6, SUB, width),
        ]
        + moments
        + frames
        + images,
        spaces={0: pltpu.SMEM},
        rows=rows,
        groups=groups,
    )
    (sums,) = call(
        gradient_kernel,
        [(2 * chains, rank)],
        [exchanged(sent), kept, state, packed, fields, early, eigenvalues[None]],
        [(rows * chains, width), (chains, rows * rank)],
        rows=rows,
        groups=groups,
    )
    steps = math.gcd(4, width // LANES)
    proposal, new_coef = call(
        proposal_kernel,
        [log_field.shape, (chains, rank)],
        [summed(sums), eigenvalues[None], subspace_noise, fields, log_field, noise_field],
        [log_field.shape, pltpu.SemaphoreType.DMA((steps,))],
        out_spaces={0: pl.ANY},
        rows=rows,
        chains=chains,
        steps=steps,
    )
    return (proposal, new_coef)


def solution(mesh):
    return jax.shard_map(
        per_device,
        mesh=mesh,
        in_specs=(
            P("rows", None),
            P("rows", None),
            P("rows", None),
            P("rows", None),
            P(None, "rows", None),
            P(None, "rows", None),
            P(),
            P(),
            P(None, "rows", None),
        ),
        out_specs=(P(None, "rows", None), P()),
        check_vma=False,
    )
```

```python
import functools
import math

import jax
import jax.numpy as jnp
from jax import lax
from jax.experimental import pallas as pl
from jax.experimental.pallas import tpu as pltpu
from jax.sharding import PartitionSpec as P

ITERS = 4
SHIFTS = (0.0, 0.75)
AXIS = "rows"
SUB, LANES = 8, 128
SUMS = 2 * ITERS * len(SHIFTS)


def shifted(value, step):
    count = lax.axis_size(AXIS)
    pairs = [(i, i + step) for i in range(count) if 0 <= i + step < count]
    return lax.ppermute(value, AXIS, pairs)


def exchanged(value):
    return lax.all_to_all(value, AXIS, 0, 0)


def summed(value):
    count = lax.axis_size(AXIS)
    if count & (count - 1):
        return lax.psum(value, AXIS)
    stride = 1
    while stride < count:
        radix = 4 if (count // stride).bit_length() & 1 else 2
        parts = [value]
        for k in range(1, radix):
            parts.append(lax.ppermute(value, AXIS, [(i, i ^ (k * stride)) for i in range(count)]))
        while len(parts) > 1:
            parts = [a + b for a, b in zip(parts[::2], parts[1::2])]
        value = parts[0]
        stride *= radix
    return value


def differences(sequence, shift):
    out = [sequence[0]]
    while len(sequence) > 1:
        if shift == 0.0:
            sequence = sequence[1:]
        elif shift == 1.0:
            sequence = [b - a for a, b in zip(sequence[:-1], sequence[1:])]
        else:
            sequence = [b - shift * a for a, b in zip(sequence[:-1], sequence[1:])]
        out.append(sequence[0])
    return out


def coefficients(sums):
    chosen, best = None, None
    for index, shift in enumerate(SHIFTS):
        eta = sums[index * 2 * ITERS : (index + 1) * 2 * ITERS]
        gram = [(1.0 - shift) * eta[k] - eta[k + 1] for k in range(2 * ITERS - 1)]
        low = [[None] * ITERS for _ in range(ITERS)]
        scaled = [[None] * ITERS for _ in range(ITERS)]
        inverse, reduced, quality = [None] * ITERS, [None] * ITERS, None
        for i in range(ITERS):
            for j in range(i):
                entry = gram[i + j]
                for k in range(j):
                    entry = entry - low[i][k] * scaled[j][k]
                scaled[i][j] = entry
                low[i][j] = entry * inverse[j]
            pivot, target = gram[2 * i], eta[i]
            for k in range(i):
                pivot = pivot - low[i][k] * scaled[i][k]
                target = target - low[i][k] * reduced[k]
            size = (1.0 - shift) * eta[2 * i] + jnp.abs(eta[2 * i + 1])
            usable = pivot > 1e-6 * gram[2 * i]
            ratio = jnp.where(usable, pivot, 0.0) / jnp.where(size > 0.0, size, 1.0)
            quality = ratio if quality is None else jnp.minimum(quality, ratio)
            inverse[i] = jnp.where(usable, 1.0 / jnp.where(usable, pivot, 1.0), 0.0)
            reduced[i] = target
        weights = [None] * ITERS
        for i in reversed(range(ITERS)):
            entry = reduced[i] * inverse[i]
            for k in range(i + 1, ITERS):
                entry = entry - low[k][i] * weights[k]
            weights[i] = entry
        if shift != 0.0:
            for step in range(ITERS - 1):
                for k in range(ITERS - 2, step - 1, -1):
                    weights[k] = weights[k] - shift * weights[k + 1]
        if chosen is None:
            chosen, best = weights, quality
        else:
            better = quality > best
            chosen = [jnp.where(better, a, b) for a, b in zip(weights, chosen)]
            best = jnp.where(better, quality, best)
    return chosen


def folds_of(groups):
    folds = SUB
    while folds * groups * SUMS > LANES:
        folds //= 2
    return folds


def krylov(vectors, images, inverse, across, along):
    width = across.shape[-1]
    groups = inverse.shape[1]
    for k in range(ITERS - 1):
        for i in range(images[k].shape[0]):
            at = i + k + 1
            for g in range(groups):
                v = vectors[k][i + 1, g]
                side = across[at]
                beside = pltpu.roll(side * v, 1, 1) + side * pltpu.roll(v, width - 1, 1)
                image = along[at] * vectors[k][i, g] + along[at + 1] * vectors[k][i + 2, g] + beside
                images[k][i, g] = image
                vectors[k + 1][i, g] = image * inverse[at, g]


def moment_tile(rows, right_side, vectors, images, thirds, halves, across, along):
    width = across.shape[-1]
    groups = vectors[0].shape[1]
    above = ITERS - 1
    for index, shift in enumerate(SHIFTS):
        for g in range(groups):
            if shift != 0.0:
                for r in range(rows + 1):
                    v = [vectors[k][r + above - k, g] for k in range(ITERS)]
                    thirds[r, g] = differences(v, shift)[ITERS - 1]
            third = thirds if shift != 0.0 else vectors[ITERS - 1]
            for r in range(rows):
                u = pltpu.roll(third[r, g], width - 1, 1)
                u = across[above + r] * u + along[above + r + 1] * third[r + 1, g]
                halves[index, r, g] = u
    lane = lax.broadcasted_iota(jnp.int32, (SUB, LANES), 1)
    tile = jnp.zeros((SUB, LANES), jnp.float32)
    for g in range(groups):

        def one_row(r, totals):
            totals = list(totals)
            for start in range(0, width, LANES):
                cut = pl.ds(start, LANES)
                v = [vectors[k][r + above - k, g, :, cut] for k in range(ITERS - 1)]
                s = [right_side(r, g, cut)]
                s += [images[k][r + above - k - 1, g, :, cut] for k in range(ITERS - 1)]
                for index, shift in enumerate(SHIFTS):
                    u, t = differences(v, shift), differences(s, shift)
                    u.append((thirds if shift != 0.0 else vectors[ITERS - 1])[r, g, :, cut])
                    t.append(halves[index, r, g, :, cut])
                    for m in range(2 * ITERS):
                        slot = index * 2 * ITERS + m
                        totals[slot] = totals[slot] + u[m // 2] * t[(m + 1) // 2]
            return tuple(totals)

        zero = jnp.zeros((SUB, LANES), jnp.float32)
        totals = list(lax.fori_loop(0, rows, one_row, (zero,) * SUMS))
        for index, shift in enumerate(SHIFTS):
            last = (index + 1) * 2 * ITERS - 1
            totals[last] = 2.0 * totals[last] - shift * totals[last - 1]
        for m, total in enumerate(totals):
            tile = jnp.where(lane == g * SUMS + m, jnp.sum(total, 1, keepdims=True), tile)
    folds = folds_of(groups)
    out = tile
    for q in range(1, folds):
        part = pltpu.roll(tile, q * (LANES // folds), 1)
        out = out + pltpu.roll(part, SUB - q * (SUB // folds), 0)
    return out[: SUB // folds]


def spread(ref, at):
    return jnp.broadcast_to(ref[at : at + 1, :], (SUB, ref.shape[-1]))


def lateral(here):
    width = here.shape[-1]
    column = lax.broadcasted_iota(jnp.int32, here.shape, 1)
    left = jnp.where(column == 0, here, pltpu.roll(here, 1, 1))
    right = jnp.where(column == width - 1, here, pltpu.roll(here, width - 1, 1))
    right = 0.5 * (here + right)
    return 0.5 * (here + left), right, jnp.where(column == width - 1, 0.0, right)


class Packed:
    def __init__(self, rows, chains):
        self.rows, self.chains = rows, chains
        self.split = (rows - 2) * chains
        self.upward = self.split
        self.downward = (rows - 1) * chains + 2 * rows

    def log(self, row, g):
        at = row * self.chains + g * SUB
        return at if row < self.rows - 2 else at + 2 * self.rows

    def source(self, row):
        return self.split + row

    def cond(self, row):
        return self.split + self.rows + row


def forward_kernel(
    _,
    place,
    own,
    before,
    after,
    far,
    sent,
    v0,
    v1,
    v2,
    v3,
    inverse,
    across,
    along,
    cond,
    side,
    thirds,
    halves,
    *images,
    rows,
    groups,
):
    halo = ITERS
    above = halo - 1
    total = rows + above + halo
    chains = groups * SUB
    spot = Packed(rows, chains)
    vectors = (v0, v1, v2, v3)
    first, last = place[0], place[1]
    for i in range(halo):
        at = spot.cond(rows - halo + i) - chains
        cond[i] = jnp.where(first == 0, spread(own, spot.cond(0)), spread(before, at))
        at = spot.cond(i)
        cond[halo + rows + i] = jnp.where(
            last == 0, spread(own, spot.cond(rows - 1)), spread(after, at)
        )
    for i in range(rows):
        cond[halo + i] = spread(own, spot.cond(i))
    cond[total + 1] = jnp.where(last == 1, spread(after, spot.cond(halo - 1)), spread(far, 0))
    for i in range(total + 1):
        along[i] = 0.5 * (cond[i] + cond[i + 1])
    for i in range(total):
        left, right, across[i] = lateral(cond[i + 1])
        edges = along[i] + along[i + 1] + left + right
        if i < above:
            ref, row, outside = before, rows - above + i, first == 0
        elif i < above + rows:
            ref, row, outside = own, i - above, None
        else:
            ref, row, outside = after, i - above - rows, last == 0
        skipped = chains if ref is before else 0
        source = spread(ref, spot.source(row) - skipped)
        if ref is own:
            side[row] = source
        for g in range(groups):
            start = spot.log(row, g) - skipped
            value = 1.0 / (edges + jnp.exp(ref[start : start + SUB, :]))
            if outside is not None:
                value = jnp.where(outside, 0.0, value)
            inverse[i, g] = value
            vectors[0][i, g] = source * value
    krylov(vectors, images, inverse, across, along)
    tile = moment_tile(
        rows, lambda r, g, cut: side[r, :, cut], vectors, images, thirds, halves, across, along
    )
    sent[...] = jnp.broadcast_to(tile[None], sent.shape)


def total_of(got):
    parts = [got[d] for d in range(got.shape[0])]
    while len(parts) > 1:
        parts = [a + b for a, b in zip(parts[::2], parts[1::2])] + parts[len(parts) & ~1 :]
    tile, folds = parts[0], SUB // parts[0].shape[0]
    tiles = [tile] + [pltpu.roll(tile, LANES - q * (LANES // folds), 1) for q in range(1, folds)]
    return jnp.concatenate(tiles, 0)


def weights_of(tile, g):
    sums = [
        jnp.broadcast_to(tile[:, g * SUMS + m : g * SUMS + m + 1], (SUB, LANES)) for m in range(SUMS)
    ]
    return [weight[:, :1] for weight in coefficients(sums)]


def adjoint_kernel(
    place,
    got,
    f0,
    f1,
    f2,
    f3,
    inverse,
    across,
    along,
    before,
    after,
    far_before,
    far_after,
    precision,
    observed,
    sent,
    kept,
    state,
    side,
    outer,
    outer_inverse,
    outer_across,
    outer_along,
    thirds,
    halves,
    *scratch,
    rows,
    groups,
):
    halo = ITERS
    above = halo - 1
    width = across.shape[-1]
    chains = groups * SUB
    spot = Packed(rows, chains)
    first, last = place[0], place[1]
    near = (f0, f1, f2, f3)
    low, high = -above, rows + halo - 1
    new_rows = [low - k for k in (3, 2, 1)] + [high + k for k in (1, 2, 3)]
    slot = {row: i for i, row in enumerate(new_rows)}

    def cond_at(row):
        if row < -rows:
            at = row + 2 * rows
            value = spread(far_before, rows + at)
            if at == rows - 1:
                value = jnp.where(first == 1, spread(before, spot.cond(0) - chains), value)
            return value
        if row < 0:
            return spread(before, spot.cond(row + rows) - chains)
        if row < 2 * rows:
            return spread(after, spot.cond(row - rows))
        return spread(far_after, spot.cond(row - 2 * rows))

    for edge in range(low - 3, low):
        outer_along[edge - low + 3] = 0.5 * (cond_at(edge - 1) + cond_at(edge))
    for edge in range(high + 2, high + 5):
        outer_along[edge - high + 1] = 0.5 * (cond_at(edge - 1) + cond_at(edge))

    def along_at(row):
        if row < low:
            return outer_along[row - low + 3]
        if row > high + 1:
            return outer_along[row - high + 1]
        return along[row - low]

    def across_at(row):
        return outer_across[slot[row]] if row in slot else across[row - low]

    def inverse_at(row, g):
        return outer_inverse[slot[row], g] if row in slot else inverse[row - low, g]

    for row in new_rows:
        left, right, outer_across[slot[row]] = lateral(cond_at(row))
        edges = along_at(row) + along_at(row + 1) + left + right
        for g in range(groups):
            if row < -rows:
                at = row + 2 * rows
                outside, source = first <= 1, spread(far_before, at)
                start = 2 * rows + (at - rows + 2) * chains + g * SUB
                log = far_before[start : start + SUB, :]
            elif row < 0:
                outside, source = first == 0, spread(before, spot.source(row + rows) - chains)
                start = 2 * rows + 2 * chains + g * SUB
                log = far_before[start : start + SUB, :]
            else:
                at = row - 2 * rows
                outside, source = last <= 1, spread(far_after, spot.source(at))
                start = spot.log(at, g)
                log = far_after[start : start + SUB, :]
            value = jnp.where(outside, 0.0, 1.0 / (edges + jnp.exp(log)))
            outer_inverse[slot[row], g] = value
            outer[0, slot[row], g] = source * value

    def vector(k, row, g):
        if row < low + k:
            return outer[k, row - low + 3 - k, g]
        if row > high - k:
            return outer[k, row - high + 2 + k, g]
        return near[k][row - low - k, g]

    for k in range(ITERS - 1):
        for i, row in enumerate([low + k + 1 - j for j in (3, 2, 1)] + [high - k - 1 + j for j in (1, 2, 3)]):
            for g in range(groups):
                v, edge = vector(k, row, g), across_at(row)
                image = pltpu.roll(edge * v, 1, 1) + edge * pltpu.roll(v, width - 1, 1)
                image = along_at(row) * vector(k, row - 1, g) + along_at(row + 1) * vector(k, row + 1, g) + image
                outer[k + 1, i, g] = image * inverse_at(row, g)

    vectors, images = scratch[:ITERS], scratch[ITERS:]
    tile = total_of(got)
    for g in range(groups):
        weights = weights_of(tile, g)
        for i in range(high - low + 1):
            row = low + i
            value = weights[0] * vector(0, row, g)
            for k in range(1, ITERS):
                value = value + weights[k] * vector(k, row, g)
            if row < 0:
                at = row + rows
                at = far_before.shape[0] - 2 * rows + at
                scale, target = spread(far_before, at), spread(far_before, at + rows)
            elif row < rows:
                state[row, g] = value
                scale, target = spread(precision, row), spread(observed, row)
            else:
                at = far_after.shape[0] - 2 * rows + row - rows
                scale, target = spread(far_after, at), spread(far_after, at + rows)
            value = scale * (value - target)
            if 0 <= row < rows:
                side[row, g] = value
            vectors[0][i, g] = value * inverse[i, g]
    krylov(vectors, images, inverse, across, along)
    tile = moment_tile(
        rows, lambda r, g, cut: side[r, g, :, cut], vectors, images, thirds, halves, across, along
    )
    sent[...] = jnp.broadcast_to(tile[None], sent.shape)
    for k in range(ITERS):
        for r in range(rows):
            for g in range(groups):
                kept[k, r, g] = vectors[k][r + above - k, g]


def factors(eigenvalues):
    variance = 1.0 / (1.0 + eigenvalues)
    below = 2.0 + 0.8 * variance
    return (2.0 - 0.8 * variance) / below, 1.6 * variance / below, jnp.sqrt(6.4 * variance) / below


def folded(picked, rows):
    size = picked.shape[1]
    lane = lax.broadcasted_iota(jnp.int32, (size, size // rows), 0)
    to = lax.broadcasted_iota(jnp.int32, (size, size // rows), 1)
    ones = jnp.where((lane >= to * rows) & (lane < to * rows + rows), 1.0, 0.0).astype(jnp.bfloat16)
    total = None
    for _ in range(3):
        part = picked.astype(jnp.bfloat16)
        picked = picked - part.astype(jnp.float32)
        part = jnp.dot(part, ones, preferred_element_type=jnp.float32)
        total = part if total is None else total + part
    return total


def picked_rows(product, rows, chains):
    row = lax.rem(lax.broadcasted_iota(jnp.int32, (chains, product.shape[1]), 1), rows)
    out = product[:chains]
    for x in range(1, rows):
        out = jnp.where(row == x, product[x * chains : (x + 1) * chains], out)
    return out


def across_lanes(left, right):
    return lax.dot_general(left, right, (((1,), (1,)), ((), ())), preferred_element_type=jnp.float32)


def early_kernel(basis, own, noise, fields, coefs, picked, *, rows, chains, steps):
    ranks = basis.shape[0] // steps
    width = basis.shape[2]
    spot = Packed(rows, chains)
    log = jnp.concatenate([own[: spot.split, :], own[spot.split + 2 * rows :, :]], 0)
    left = jnp.concatenate([log.astype(jnp.bfloat16), noise[...]], 0)
    for j in range(steps):
        block = basis[pl.ds(j * ranks, ranks)].reshape(ranks * rows, width)
        cut = pl.ds(j * ranks * rows, ranks * rows)
        fields[cut, :] = block
        product = across_lanes(left, block)
        half = rows * chains
        picked[:chains, cut] = picked_rows(product[:half], rows, chains)
        picked[chains:, cut] = picked_rows(product[half:], rows, chains)
    coefs[...] = folded(picked[...], rows)


def gradient_kernel(
    got, kept, state, log, fields, early, eigenvalues, sums, gradient, picked, *, rows, groups
):
    tile = total_of(got)
    chains = groups * SUB
    spot = Packed(rows, chains)
    for g in range(groups):
        weights = weights_of(tile, g)
        for r in range(rows):
            value = weights[0] * kept[0, r, g]
            for k in range(1, ITERS):
                value = value + weights[k] * kept[k, r, g]
            at = spot.log(r, g)
            value = -jnp.exp(log[at : at + SUB, :]) * value * state[r, g]
            at = r * chains + g * SUB
            gradient[at : at + SUB, :] = value
    left = gradient[...].astype(jnp.bfloat16)
    size = fields.shape[0]
    step = min(size, 2 * LANES)
    for start in range(0, size, step):
        product = across_lanes(left, fields[start : start + step, :])
        picked[:, start : start + step] = picked_rows(product, rows, chains)
    keep, drift, _ = factors(eigenvalues[...])
    state_coef, noise_coef = early[:chains], early[chains:]
    sums[:chains] = keep * state_coef - drift * folded(picked[...], rows)
    sums[chains:] = -0.6 * state_coef - 0.8 * noise_coef


def proposal_kernel(
    sums, eigenvalues, subspace, fields, log, noise, proposal, new_coef, result, sent, *, rows, chains, steps
):
    _, _, noise_factor = factors(eigenvalues[...])
    coef = sums[:chains] + noise_factor * subspace[...]
    new_coef[...] = coef
    correction = (coef + sums[chains:]).astype(jnp.bfloat16)
    size, width = fields.shape
    rank = size // rows
    row = lax.broadcasted_iota(jnp.int32, (chains * rows, chains), 0)
    to = lax.broadcasted_iota(jnp.int32, (chains * rows, chains), 1)
    tall = jnp.where((row >= to * rows) & (row < to * rows + rows), 1.0, 0.0).astype(jnp.bfloat16)
    lane = lax.broadcasted_iota(jnp.int32, (rank, size), 1)
    to = lax.broadcasted_iota(jnp.int32, (rank, size), 0)
    wide = jnp.where((lane >= to * rows) & (lane < to * rows + rows), 1.0, 0.0).astype(jnp.bfloat16)
    left = jnp.dot(tall, correction, preferred_element_type=jnp.float32).astype(jnp.bfloat16)
    left = jnp.dot(left, wide, preferred_element_type=jnp.float32)
    row = lax.rem(lax.broadcasted_iota(jnp.int32, left.shape, 0), rows)
    lane = lax.rem(lax.broadcasted_iota(jnp.int32, left.shape, 1), rows)
    left = jnp.where(row == lane, left, 0.0).astype(jnp.bfloat16)
    copies = []
    for j in range(steps):
        cut = pl.ds(j * (width // steps), width // steps)
        product = jnp.dot(left, fields[:, cut], preferred_element_type=jnp.float32)
        for c in range(chains):
            base = 0.6 * log[c, :, cut] + 0.8 * noise[c, :, cut]
            result[c, :, cut] = base + product[c * rows : (c + 1) * rows]
        copies.append(
            pltpu.make_async_copy(result.at[:, :, cut], proposal.at[:, :, cut], sent.at[j])
        )
        copies[-1].start()
    for copy in copies:
        copy.wait()


def call(kernel, outs, args, scratch=(), spaces=(), out_spaces=(), **static):
    spaces = dict(spaces)
    out_spaces = dict(out_spaces)
    sizes = [math.prod(s) * 4 if isinstance(s, tuple) else 0 for s in scratch]
    limit = sum(sizes) + static.pop("more", 0) + 3 * 1024 * 1024
    outs = [out if len(out) == 2 and not isinstance(out[0], int) else (out, jnp.float32) for out in outs]
    return pl.pallas_call(
        functools.partial(kernel, **static),
        out_shape=[jax.ShapeDtypeStruct(*out) for out in outs],
        in_specs=[pl.BlockSpec(memory_space=spaces.get(i, pltpu.VMEM)) for i in range(len(args))],
        out_specs=[pl.BlockSpec(memory_space=out_spaces.get(i, pltpu.VMEM)) for i in range(len(outs))],
        scratch_shapes=[pltpu.VMEM(s, jnp.float32) if isinstance(s, tuple) else s for s in scratch],
        compiler_params=pltpu.CompilerParams(vmem_limit_bytes=limit),
    )(*args)


def per_device(
    source,
    observed,
    precision,
    conductivity,
    log_field,
    noise_field,
    subspace_noise,
    eigenvalues,
    basis,
):
    halo = ITERS
    chains, rows, width = log_field.shape
    rank = basis.shape[0]
    groups = chains // SUB
    position = lax.axis_index(AXIS)
    devices = lax.axis_size(AXIS)

    assert rows == halo and chains % SUB == 0
    above = halo - 1
    spot = Packed(rows, chains)
    far = shifted(conductivity[:1], -2)
    place = jnp.stack([position, devices - 1 - position])
    log_rows = jnp.transpose(log_field, (1, 0, 2)).reshape(rows * chains, width)
    packed = jnp.concatenate(
        [log_rows[: spot.split], source, conductivity, log_rows[spot.split :]], 0
    )
    before = shifted(packed[chains:], 1)
    after = shifted(packed, -1)
    noise_rows = jnp.transpose(noise_field, (1, 0, 2)).astype(jnp.bfloat16)
    steps = math.gcd(8, rank)
    fields, early = call(
        early_kernel,
        [((rows * rank, width), jnp.bfloat16), (2 * chains, rank)],
        [
            basis,
            packed,
            noise_rows.reshape(rows * chains, width),
        ],
        [(2 * chains, rows * rank)],
        rows=rows,
        chains=chains,
        steps=steps,
    )
    early, precision, observed = lax.optimization_barrier((early, precision, observed))
    far_before = [before[spot.upward - chains :], packed[:chains], precision, observed]
    far_before = jnp.concatenate(far_before, 0)
    far_after = jnp.concatenate([after[: spot.downward], precision, observed], 0)
    far_before = shifted(far_before, 1)
    far_after = shifted(far_after, -1)

    total = rows + above + halo
    block = (groups, SUB, width)
    tiles = (devices, SUB // folds_of(groups), LANES)
    moments = [(rows + 1,) + block, (len(SHIFTS), rows) + block]
    frames = [(total - 2 * k,) + block for k in range(ITERS)]
    images = [(total - 2 * k - 2,) + block for k in range(ITERS - 1)]
    sent, *vectors, inverse, across, along = call(
        forward_kernel,
        [tiles] + frames + [(total,) + block, (total, SUB, width), (total + 1, SUB, width)],
        [early, place, packed, before, after, far],
        [(total + 2, SUB, width), (rows, SUB, width)] + moments + images,
        spaces={1: pltpu.SMEM},
        rows=rows,
        groups=groups,
    )
    sent, kept, state = call(
        adjoint_kernel,
        [tiles, (ITERS, rows) + block, (rows,) + block],
        [place, exchanged(sent), *vectors, inverse, across, along]
        + [before, after, far_before, far_after, precision, observed],
        [
            (rows,) + block,
            (ITERS, 6) + block,
            (6,) + block,
            (6, SUB, width),
            (6, SUB, width),
        ]
        + moments
        + frames
        + images,
        spaces={0: pltpu.SMEM},
        rows=rows,
        groups=groups,
    )
    (sums,) = call(
        gradient_kernel,
        [(2 * chains, rank)],
        [exchanged(sent), kept, state, packed, fields, early, eigenvalues[None]],
        [(rows * chains, width), (chains, rows * rank)],
        rows=rows,
        groups=groups,
    )
    steps = math.gcd(4, width // LANES)
    proposal, new_coef = call(
        proposal_kernel,
        [log_field.shape, (chains, rank)],
        [summed(sums), eigenvalues[None], subspace_noise, fields, log_field, noise_field],
        [log_field.shape, pltpu.SemaphoreType.DMA((steps,))],
        out_spaces={0: pl.ANY},
        rows=rows,
        chains=chains,
        steps=steps,
    )
    return (proposal, new_coef)


def solution(mesh):
    return jax.shard_map(
        per_device,
        mesh=mesh,
        in_specs=(
            P("rows", None),
            P("rows", None),
            P("rows", None),
            P("rows", None),
            P(None, "rows", None),
            P(None, "rows", None),
            P(),
            P(),
            P(None, "rows", None),
        ),
        out_specs=(P(None, "rows", None), P()),
        check_vma=False,
    )
```

```python
import functools
import math

import jax
import jax.numpy as jnp
from jax import lax
from jax.experimental import pallas as pl
from jax.experimental.pallas import tpu as pltpu
from jax.sharding import PartitionSpec as P

ITERS = 4
SHIFTS = (0.0, 0.75)
AXIS = "rows"
SUB, LANES = 8, 128
SUMS = 2 * ITERS * len(SHIFTS)


def shifted(value, step):
    count = lax.axis_size(AXIS)
    pairs = [(i, i + step) for i in range(count) if 0 <= i + step < count]
    return lax.ppermute(value, AXIS, pairs)


def exchanged(value):
    return lax.all_to_all(value, AXIS, 0, 0)


def summed(value):
    count = lax.axis_size(AXIS)
    if count & (count - 1):
        return lax.psum(value, AXIS)
    stride = 1
    while stride < count:
        radix = 4 if (count // stride).bit_length() & 1 else 2
        parts = [value]
        for k in range(1, radix):
            parts.append(lax.ppermute(value, AXIS, [(i, i ^ (k * stride)) for i in range(count)]))
        while len(parts) > 1:
            parts = [a + b for a, b in zip(parts[::2], parts[1::2])]
        value = parts[0]
        stride *= radix
    return value


def differences(sequence, shift):
    out = [sequence[0]]
    while len(sequence) > 1:
        if shift == 0.0:
            sequence = sequence[1:]
        elif shift == 1.0:
            sequence = [b - a for a, b in zip(sequence[:-1], sequence[1:])]
        else:
            sequence = [b - shift * a for a, b in zip(sequence[:-1], sequence[1:])]
        out.append(sequence[0])
    return out


def coefficients(sums):
    chosen, best = None, None
    for index, shift in enumerate(SHIFTS):
        eta = sums[index * 2 * ITERS : (index + 1) * 2 * ITERS]
        gram = [(1.0 - shift) * eta[k] - eta[k + 1] for k in range(2 * ITERS - 1)]
        low = [[None] * ITERS for _ in range(ITERS)]
        scaled = [[None] * ITERS for _ in range(ITERS)]
        inverse, reduced, quality = [None] * ITERS, [None] * ITERS, None
        for i in range(ITERS):
            for j in range(i):
                entry = gram[i + j]
                for k in range(j):
                    entry = entry - low[i][k] * scaled[j][k]
                scaled[i][j] = entry
                low[i][j] = entry * inverse[j]
            pivot, target = gram[2 * i], eta[i]
            for k in range(i):
                pivot = pivot - low[i][k] * scaled[i][k]
                target = target - low[i][k] * reduced[k]
            size = (1.0 - shift) * eta[2 * i] + jnp.abs(eta[2 * i + 1])
            usable = pivot > 1e-6 * gram[2 * i]
            ratio = jnp.where(usable, pivot, 0.0) / jnp.where(size > 0.0, size, 1.0)
            quality = ratio if quality is None else jnp.minimum(quality, ratio)
            inverse[i] = jnp.where(usable, 1.0 / jnp.where(usable, pivot, 1.0), 0.0)
            reduced[i] = target
        weights = [None] * ITERS
        for i in reversed(range(ITERS)):
            entry = reduced[i] * inverse[i]
            for k in range(i + 1, ITERS):
                entry = entry - low[k][i] * weights[k]
            weights[i] = entry
        if shift != 0.0:
            for step in range(ITERS - 1):
                for k in range(ITERS - 2, step - 1, -1):
                    weights[k] = weights[k] - shift * weights[k + 1]
        if chosen is None:
            chosen, best = weights, quality
        else:
            better = quality > best
            chosen = [jnp.where(better, a, b) for a, b in zip(weights, chosen)]
            best = jnp.where(better, quality, best)
    return chosen


def folds_of(groups):
    folds = SUB
    while folds * groups * SUMS > LANES:
        folds //= 2
    return folds


def krylov(rows, vectors, images, inverse, across, along):
    width = across.shape[-1]
    groups = inverse.shape[1]
    for k in range(ITERS - 1):
        for i in range(images[k].shape[0]):
            at = i + k + 1
            for g in range(groups):
                v = vectors[k][i + 1, g]
                side = across[at]
                beside = pltpu.roll(side * v, 1, 1) + side * pltpu.roll(v, width - 1, 1)
                image = along[at] * vectors[k][i, g] + along[at + 1] * vectors[k][i + 2, g] + beside
                if 0 <= i + k + 2 - ITERS < rows:
                    images[k][i, g] = image
                vectors[k + 1][i, g] = image * inverse[at, g]


def moment_tile(rows, right_side, vectors, images, thirds, halves, across, along):
    width = across.shape[-1]
    groups = vectors[0].shape[1]
    above = ITERS - 1
    for index, shift in enumerate(SHIFTS):
        for g in range(groups):
            if shift != 0.0:
                for r in range(rows + 1):
                    v = [vectors[k][r + above - k, g] for k in range(ITERS)]
                    thirds[r, g] = differences(v, shift)[ITERS - 1]
            third = thirds if shift != 0.0 else vectors[ITERS - 1]
            for r in range(rows):
                u = pltpu.roll(third[r, g], width - 1, 1)
                u = across[above + r] * u + along[above + r + 1] * third[r + 1, g]
                halves[index, r, g] = u
    lane = lax.broadcasted_iota(jnp.int32, (SUB, LANES), 1)
    tile = jnp.zeros((SUB, LANES), jnp.float32)
    for g in range(groups):

        def one_row(r, totals):
            totals = list(totals)
            for start in range(0, width, LANES):
                cut = pl.ds(start, LANES)
                v = [vectors[k][r + above - k, g, :, cut] for k in range(ITERS - 1)]
                s = [right_side(r, g, cut)]
                s += [images[k][r + above - k - 1, g, :, cut] for k in range(ITERS - 1)]
                for index, shift in enumerate(SHIFTS):
                    u, t = differences(v, shift), differences(s, shift)
                    u.append((thirds if shift != 0.0 else vectors[ITERS - 1])[r, g, :, cut])
                    t.append(halves[index, r, g, :, cut])
                    for m in range(2 * ITERS):
                        slot = index * 2 * ITERS + m
                        totals[slot] = totals[slot] + u[m // 2] * t[(m + 1) // 2]
            return tuple(totals)

        zero = jnp.zeros((SUB, LANES), jnp.float32)
        totals = list(lax.fori_loop(0, rows, one_row, (zero,) * SUMS))
        for index, shift in enumerate(SHIFTS):
            last = (index + 1) * 2 * ITERS - 1
            totals[last] = 2.0 * totals[last] - shift * totals[last - 1]
        for m, total in enumerate(totals):
            tile = jnp.where(lane == g * SUMS + m, jnp.sum(total, 1, keepdims=True), tile)
    folds = folds_of(groups)
    out = tile
    for q in range(1, folds):
        part = pltpu.roll(tile, q * (LANES // folds), 1)
        out = out + pltpu.roll(part, SUB - q * (SUB // folds), 0)
    return out[: SUB // folds]


def spread(ref, at):
    return jnp.broadcast_to(ref[at : at + 1, :], (SUB, ref.shape[-1]))


def lateral(here):
    width = here.shape[-1]
    column = lax.broadcasted_iota(jnp.int32, here.shape, 1)
    left = jnp.where(column == 0, here, pltpu.roll(here, 1, 1))
    right = jnp.where(column == width - 1, here, pltpu.roll(here, width - 1, 1))
    right = 0.5 * (here + right)
    return 0.5 * (here + left), right, jnp.where(column == width - 1, 0.0, right)


class Packed:
    def __init__(self, rows, chains):
        self.rows, self.chains = rows, chains
        self.split = (rows - 2) * chains
        self.upward = self.split
        self.downward = (rows - 1) * chains + 2 * rows

    def log(self, row, g):
        at = row * self.chains + g * SUB
        return at if row < self.rows - 2 else at + 2 * self.rows

    def source(self, row):
        return self.split + row

    def cond(self, row):
        return self.split + self.rows + row


def forward_kernel(
    _,
    place,
    own,
    before,
    after,
    far,
    sent,
    v0,
    v1,
    v2,
    v3,
    inverse,
    across,
    along,
    cond,
    side,
    thirds,
    halves,
    *images,
    rows,
    groups,
):
    halo = ITERS
    above = halo - 1
    total = rows + above + halo
    chains = groups * SUB
    spot = Packed(rows, chains)
    vectors = (v0, v1, v2, v3)
    first, last = place[0], place[1]
    for i in range(halo):
        at = spot.cond(rows - halo + i) - chains
        cond[i] = jnp.where(first == 0, spread(own, spot.cond(0)), spread(before, at))
        at = spot.cond(i)
        cond[halo + rows + i] = jnp.where(
            last == 0, spread(own, spot.cond(rows - 1)), spread(after, at)
        )
    for i in range(rows):
        cond[halo + i] = spread(own, spot.cond(i))
    cond[total + 1] = jnp.where(last == 1, spread(after, spot.cond(halo - 1)), spread(far, 0))
    for i in range(total + 1):
        along[i] = 0.5 * (cond[i] + cond[i + 1])
    for i in range(total):
        left, right, across[i] = lateral(cond[i + 1])
        edges = along[i] + along[i + 1] + left + right
        if i < above:
            ref, row, outside = before, rows - above + i, first == 0
        elif i < above + rows:
            ref, row, outside = own, i - above, None
        else:
            ref, row, outside = after, i - above - rows, last == 0
        skipped = chains if ref is before else 0
        source = spread(ref, spot.source(row) - skipped)
        if ref is own:
            side[row] = source
        for g in range(groups):
            start = spot.log(row, g) - skipped
            value = 1.0 / (edges + jnp.exp(ref[start : start + SUB, :]))
            if outside is not None:
                value = jnp.where(outside, 0.0, value)
            inverse[i, g] = value
            vectors[0][i, g] = source * value
    krylov(rows, vectors, images, inverse, across, along)
    tile = moment_tile(
        rows, lambda r, g, cut: side[r, :, cut], vectors, images, thirds, halves, across, along
    )
    sent[...] = jnp.broadcast_to(tile[None], sent.shape)


def total_of(got):
    parts = [got[d] for d in range(got.shape[0])]
    while len(parts) > 1:
        parts = [a + b for a, b in zip(parts[::2], parts[1::2])] + parts[len(parts) & ~1 :]
    tile, folds = parts[0], SUB // parts[0].shape[0]
    tiles = [tile] + [pltpu.roll(tile, LANES - q * (LANES // folds), 1) for q in range(1, folds)]
    return jnp.concatenate(tiles, 0)


def weights_of(tile, g):
    sums = [
        jnp.broadcast_to(tile[:, g * SUMS + m : g * SUMS + m + 1], (SUB, LANES)) for m in range(SUMS)
    ]
    return [weight[:, :1] for weight in coefficients(sums)]


def adjoint_kernel(
    place,
    got,
    f0,
    f1,
    f2,
    f3,
    inverse,
    across,
    along,
    before,
    after,
    far_before,
    far_after,
    precision,
    observed,
    sent,
    w0,
    w1,
    w2,
    w3,
    state,
    side,
    outer,
    outer_inverse,
    outer_across,
    outer_along,
    thirds,
    halves,
    *scratch,
    rows,
    groups,
):
    halo = ITERS
    above = halo - 1
    width = across.shape[-1]
    chains = groups * SUB
    spot = Packed(rows, chains)
    first, last = place[0], place[1]
    near = (f0, f1, f2, f3)
    low, high = -above, rows + halo - 1
    new_rows = [low - k for k in (3, 2, 1)] + [high + k for k in (1, 2, 3)]
    slot = {row: i for i, row in enumerate(new_rows)}

    def cond_at(row):
        if row < -rows:
            at = row + 2 * rows
            value = spread(far_before, rows + at)
            if at == rows - 1:
                value = jnp.where(first == 1, spread(before, spot.cond(0) - chains), value)
            return value
        if row < 0:
            return spread(before, spot.cond(row + rows) - chains)
        if row < 2 * rows:
            return spread(after, spot.cond(row - rows))
        return spread(far_after, spot.cond(row - 2 * rows))

    for edge in range(low - 3, low):
        outer_along[edge - low + 3] = 0.5 * (cond_at(edge - 1) + cond_at(edge))
    for edge in range(high + 2, high + 5):
        outer_along[edge - high + 1] = 0.5 * (cond_at(edge - 1) + cond_at(edge))

    def along_at(row):
        if row < low:
            return outer_along[row - low + 3]
        if row > high + 1:
            return outer_along[row - high + 1]
        return along[row - low]

    def across_at(row):
        return outer_across[slot[row]] if row in slot else across[row - low]

    def inverse_at(row, g):
        return outer_inverse[slot[row], g] if row in slot else inverse[row - low, g]

    for row in new_rows:
        left, right, outer_across[slot[row]] = lateral(cond_at(row))
        edges = along_at(row) + along_at(row + 1) + left + right
        for g in range(groups):
            if row < -rows:
                at = row + 2 * rows
                outside, source = first <= 1, spread(far_before, at)
                start = 2 * rows + (at - rows + 2) * chains + g * SUB
                log = far_before[start : start + SUB, :]
            elif row < 0:
                outside, source = first == 0, spread(before, spot.source(row + rows) - chains)
                start = 2 * rows + 2 * chains + g * SUB
                log = far_before[start : start + SUB, :]
            else:
                at = row - 2 * rows
                outside, source = last <= 1, spread(far_after, spot.source(at))
                start = spot.log(at, g)
                log = far_after[start : start + SUB, :]
            value = jnp.where(outside, 0.0, 1.0 / (edges + jnp.exp(log)))
            outer_inverse[slot[row], g] = value
            outer[0, slot[row], g] = source * value

    def vector(k, row, g):
        if row < low + k:
            return outer[k, row - low + 3 - k, g]
        if row > high - k:
            return outer[k, row - high + 2 + k, g]
        return near[k][row - low - k, g]

    for k in range(ITERS - 1):
        for i, row in enumerate([low + k + 1 - j for j in (3, 2, 1)] + [high - k - 1 + j for j in (1, 2, 3)]):
            for g in range(groups):
                v, edge = vector(k, row, g), across_at(row)
                image = pltpu.roll(edge * v, 1, 1) + edge * pltpu.roll(v, width - 1, 1)
                image = along_at(row) * vector(k, row - 1, g) + along_at(row + 1) * vector(k, row + 1, g) + image
                outer[k + 1, i, g] = image * inverse_at(row, g)

    vectors, images = (w0, w1, w2, w3), scratch
    tile = total_of(got)
    for g in range(groups):
        weights = weights_of(tile, g)
        for i in range(high - low + 1):
            row = low + i
            value = weights[0] * vector(0, row, g)
            for k in range(1, ITERS):
                value = value + weights[k] * vector(k, row, g)
            if row < 0:
                at = row + rows
                at = far_before.shape[0] - 2 * rows + at
                scale, target = spread(far_before, at), spread(far_before, at + rows)
            elif row < rows:
                state[row, g] = value
                scale, target = spread(precision, row), spread(observed, row)
            else:
                at = far_after.shape[0] - 2 * rows + row - rows
                scale, target = spread(far_after, at), spread(far_after, at + rows)
            value = scale * (value - target)
            if 0 <= row < rows:
                side[row, g] = value
            vectors[0][i, g] = value * inverse[i, g]
    krylov(rows, vectors, images, inverse, across, along)
    tile = moment_tile(
        rows, lambda r, g, cut: side[r, g, :, cut], vectors, images, thirds, halves, across, along
    )
    sent[...] = jnp.broadcast_to(tile[None], sent.shape)


def factors(eigenvalues):
    variance = 1.0 / (1.0 + eigenvalues)
    below = 2.0 + 0.8 * variance
    return (2.0 - 0.8 * variance) / below, 1.6 * variance / below, jnp.sqrt(6.4 * variance) / below


def folded(picked, rows):
    size = picked.shape[1]
    lane = lax.broadcasted_iota(jnp.int32, (size, size // rows), 0)
    to = lax.broadcasted_iota(jnp.int32, (size, size // rows), 1)
    ones = jnp.where((lane >= to * rows) & (lane < to * rows + rows), 1.0, 0.0).astype(jnp.bfloat16)
    total = None
    for _ in range(3):
        part = picked.astype(jnp.bfloat16)
        picked = picked - part.astype(jnp.float32)
        part = jnp.dot(part, ones, preferred_element_type=jnp.float32)
        total = part if total is None else total + part
    return total


def picked_rows(product, rows, chains):
    row = lax.rem(lax.broadcasted_iota(jnp.int32, (chains, product.shape[1]), 1), rows)
    out = product[:chains]
    for x in range(1, rows):
        out = jnp.where(row == x, product[x * chains : (x + 1) * chains], out)
    return out


def across_lanes(left, right):
    return lax.dot_general(left, right, (((1,), (1,)), ((), ())), preferred_element_type=jnp.float32)


def early_kernel(basis, own, noise, fields, coefs, picked, *, rows, chains, steps):
    ranks = basis.shape[0] // steps
    width = basis.shape[2]
    spot = Packed(rows, chains)
    log = jnp.concatenate([own[: spot.split, :], own[spot.split + 2 * rows :, :]], 0)
    left = jnp.concatenate([log.astype(jnp.bfloat16), noise[...]], 0)
    for j in range(steps):
        block = basis[pl.ds(j * ranks, ranks)].reshape(ranks * rows, width)
        cut = pl.ds(j * ranks * rows, ranks * rows)
        fields[cut, :] = block
        product = across_lanes(left, block)
        half = rows * chains
        picked[:chains, cut] = picked_rows(product[:half], rows, chains)
        picked[chains:, cut] = picked_rows(product[half:], rows, chains)
    coefs[...] = folded(picked[...], rows)


def gradient_kernel(
    got, w0, w1, w2, w3, state, log, fields, early, eigenvalues, sums, gradient, picked, *, rows, groups
):
    tile = total_of(got)
    chains = groups * SUB
    spot = Packed(rows, chains)
    for g in range(groups):
        weights = weights_of(tile, g)
        for r in range(rows):
            value = weights[0] * w0[r + ITERS - 1, g]
            for k in range(1, ITERS):
                value = value + weights[k] * (w0, w1, w2, w3)[k][r + ITERS - 1 - k, g]
            at = spot.log(r, g)
            value = -jnp.exp(log[at : at + SUB, :]) * value * state[r, g]
            at = r * chains + g * SUB
            gradient[at : at + SUB, :] = value
    left = gradient[...].astype(jnp.bfloat16)
    size = fields.shape[0]
    step = min(size, 2 * LANES)
    for start in range(0, size, step):
        product = across_lanes(left, fields[start : start + step, :])
        picked[:, start : start + step] = picked_rows(product, rows, chains)
    keep, drift, _ = factors(eigenvalues[...])
    state_coef, noise_coef = early[:chains], early[chains:]
    sums[:chains] = keep * state_coef - drift * folded(picked[...], rows)
    sums[chains:] = -0.6 * state_coef - 0.8 * noise_coef


def proposal_kernel(
    sums, eigenvalues, subspace, fields, log, noise, proposal, new_coef, result, sent, *, rows, chains, steps
):
    _, _, noise_factor = factors(eigenvalues[...])
    coef = sums[:chains] + noise_factor * subspace[...]
    new_coef[...] = coef
    correction = (coef + sums[chains:]).astype(jnp.bfloat16)
    size, width = fields.shape
    rank = size // rows
    row = lax.broadcasted_iota(jnp.int32, (chains * rows, chains), 0)
    to = lax.broadcasted_iota(jnp.int32, (chains * rows, chains), 1)
    tall = jnp.where((row >= to * rows) & (row < to * rows + rows), 1.0, 0.0).astype(jnp.bfloat16)
    lane = lax.broadcasted_iota(jnp.int32, (rank, size), 1)
    to = lax.broadcasted_iota(jnp.int32, (rank, size), 0)
    wide = jnp.where((lane >= to * rows) & (lane < to * rows + rows), 1.0, 0.0).astype(jnp.bfloat16)
    left = jnp.dot(tall, correction, preferred_element_type=jnp.float32).astype(jnp.bfloat16)
    left = jnp.dot(left, wide, preferred_element_type=jnp.float32)
    row = lax.rem(lax.broadcasted_iota(jnp.int32, left.shape, 0), rows)
    lane = lax.rem(lax.broadcasted_iota(jnp.int32, left.shape, 1), rows)
    left = jnp.where(row == lane, left, 0.0).astype(jnp.bfloat16)
    copies = []
    for j in range(steps):
        cut = pl.ds(j * (width // steps), width // steps)
        product = jnp.dot(left, fields[:, cut], preferred_element_type=jnp.float32)
        for c in range(chains):
            base = 0.6 * log[c, :, cut] + 0.8 * noise[c, :, cut]
            result[c, :, cut] = base + product[c * rows : (c + 1) * rows]
        copies.append(
            pltpu.make_async_copy(result.at[:, :, cut], proposal.at[:, :, cut], sent.at[j])
        )
        copies[-1].start()
    for copy in copies:
        copy.wait()


def call(kernel, outs, args, scratch=(), spaces=(), out_spaces=(), **static):
    spaces = dict(spaces)
    out_spaces = dict(out_spaces)
    sizes = [math.prod(s) * 4 if isinstance(s, tuple) else 0 for s in scratch]
    limit = sum(sizes) + static.pop("more", 0) + 3 * 1024 * 1024
    outs = [out if len(out) == 2 and not isinstance(out[0], int) else (out, jnp.float32) for out in outs]
    return pl.pallas_call(
        functools.partial(kernel, **static),
        out_shape=[jax.ShapeDtypeStruct(*out) for out in outs],
        in_specs=[pl.BlockSpec(memory_space=spaces.get(i, pltpu.VMEM)) for i in range(len(args))],
        out_specs=[pl.BlockSpec(memory_space=out_spaces.get(i, pltpu.VMEM)) for i in range(len(outs))],
        scratch_shapes=[pltpu.VMEM(s, jnp.float32) if isinstance(s, tuple) else s for s in scratch],
        compiler_params=pltpu.CompilerParams(vmem_limit_bytes=limit),
    )(*args)


def per_device(
    source,
    observed,
    precision,
    conductivity,
    log_field,
    noise_field,
    subspace_noise,
    eigenvalues,
    basis,
):
    halo = ITERS
    chains, rows, width = log_field.shape
    rank = basis.shape[0]
    groups = chains // SUB
    position = lax.axis_index(AXIS)
    devices = lax.axis_size(AXIS)

    assert rows == halo and chains % SUB == 0
    above = halo - 1
    spot = Packed(rows, chains)
    far = shifted(conductivity[:1], -2)
    place = jnp.stack([position, devices - 1 - position])
    log_rows = jnp.transpose(log_field, (1, 0, 2)).reshape(rows * chains, width)
    packed = jnp.concatenate(
        [log_rows[: spot.split], source, conductivity, log_rows[spot.split :]], 0
    )
    before = shifted(packed[chains:], 1)
    after = shifted(packed, -1)
    noise_rows = jnp.transpose(noise_field, (1, 0, 2)).astype(jnp.bfloat16)
    steps = math.gcd(8, rank)
    fields, early = call(
        early_kernel,
        [((rows * rank, width), jnp.bfloat16), (2 * chains, rank)],
        [
            basis,
            packed,
            noise_rows.reshape(rows * chains, width),
        ],
        [(2 * chains, rows * rank)],
        rows=rows,
        chains=chains,
        steps=steps,
    )
    early, precision, observed = lax.optimization_barrier((early, precision, observed))
    far_before = [before[spot.upward - chains :], packed[:chains], precision, observed]
    far_before = jnp.concatenate(far_before, 0)
    far_after = jnp.concatenate([after[: spot.downward], precision, observed], 0)
    far_before = shifted(far_before, 1)
    far_after = shifted(far_after, -1)

    total = rows + above + halo
    block = (groups, SUB, width)
    tiles = (devices, SUB // folds_of(groups), LANES)
    moments = [(rows + 1,) + block, (len(SHIFTS), rows) + block]
    frames = [(total - 2 * k,) + block for k in range(ITERS)]
    images = [(total - 2 * k - 2,) + block for k in range(ITERS - 1)]
    sent, *vectors, inverse, across, along = call(
        forward_kernel,
        [tiles] + frames + [(total,) + block, (total, SUB, width), (total + 1, SUB, width)],
        [early, place, packed, before, after, far],
        [(total + 2, SUB, width), (rows, SUB, width)] + moments + images,
        spaces={1: pltpu.SMEM},
        rows=rows,
        groups=groups,
    )
    sent, *solved, state = call(
        adjoint_kernel,
        [tiles] + frames + [(rows,) + block],
        [place, exchanged(sent), *vectors, inverse, across, along]
        + [before, after, far_before, far_after, precision, observed],
        [
            (rows,) + block,
            (ITERS, 6) + block,
            (6,) + block,
            (6, SUB, width),
            (6, SUB, width),
        ]
        + moments
        + images,
        spaces={0: pltpu.SMEM},
        rows=rows,
        groups=groups,
    )
    (sums,) = call(
        gradient_kernel,
        [(2 * chains, rank)],
        [exchanged(sent), *solved, state, packed, fields, early, eigenvalues[None]],
        [(rows * chains, width), (chains, rows * rank)],
        rows=rows,
        groups=groups,
    )
    steps = math.gcd(4, width // LANES)
    proposal, new_coef = call(
        proposal_kernel,
        [log_field.shape, (chains, rank)],
        [summed(sums), eigenvalues[None], subspace_noise, fields, log_field, noise_field],
        [log_field.shape, pltpu.SemaphoreType.DMA((steps,))],
        out_spaces={0: pl.ANY},
        rows=rows,
        chains=chains,
        steps=steps,
    )
    return (proposal, new_coef)


def solution(mesh):
    return jax.shard_map(
        per_device,
        mesh=mesh,
        in_specs=(
            P("rows", None),
            P("rows", None),
            P("rows", None),
            P("rows", None),
            P(None, "rows", None),
            P(None, "rows", None),
            P(),
            P(),
            P(None, "rows", None),
        ),
        out_specs=(P(None, "rows", None), P()),
        check_vma=False,
    )
```
